32 devices in a mesh: section: 4 (over y, x), chan: 8 (over z, core).
Axes of the slice: x: 2, y: 2, z: 4, core: 2. Of those that a mesh axis runs over, the one named last changes fastest.
Arguments:
- voltages: bfloat16 [2, 512, 524288], P(None, 'chan', 'section'), may hold values from -6 to 6
- usable: int32 [4096, 512], P(('section', 'chan')), may hold values 0 or 1
- auto_power: float32 [4096, 512], P(('section', 'chan')), may hold values from 0.5 to 4
Outputs:
- gains: float32 [2, 4096, 512], P(None, ('section', 'chan'))
The draws below stay inside these ranges and needn't reach their ends.
Inputs may be any that keep to these rules, and one draw needn't show every extreme that they name: 1 marks a feed as usable in that channel, 0 as flagged.
All inputs are finite; a program needn't handle non-finite values. No bound on the sum of `usable` on one device may be relied on, other than what follows from the above.
Results may differ from the reference program's by a relative error of at most 0.0046.
Values may be sent and summed in bfloat16 or wider, within the bound.
A program may use at most 576 MiB of HBM per device.

```python
import math
import jax
import jax.numpy as jnp
from jax import lax

FEEDS = 512
CHANNELS = 4096
TAPS = 4
ITERS = 5
SPECTRA = 128
SAMPLES = 524288
N_SECTION = 4
N_CHAN = 8


def with_ends(array, rng, low, top_value):
    longest = array.shape.index(max(array.shape))
    spots = []
    for shift in (0, 1):
        where = [jax.random.randint(jax.random.fold_in(rng, axis), (), 0, length) for axis, length in enumerate(array.shape)]
        where[longest] = (where[longest] + shift) % array.shape[longest]
        spots.append(tuple(where))
    return array.at[spots[0]].set(low).at[spots[1]].set(top_value)


def levels(own_key, dims, cuts, least, top_value):
    level = 1.0
    for axis_at, parts in cuts:
        steps = jax.random.uniform(jax.random.fold_in(jax.random.fold_in(own_key, 6), axis_at), (parts,), jnp.float32, least / len(cuts), top_value / len(cuts))
        level = level * jnp.repeat(jnp.exp(steps), dims[axis_at] // parts).reshape((-1,) + (1,) * (len(dims) - 1 - axis_at))
    return level


def normal_values(stream_key, dims, spread, bound, cuts=(), held_as=jnp.bfloat16):
    values = jax.random.normal(stream_key, dims, jnp.float32) * spread
    if len(cuts) > 0:
        values = levels(stream_key, dims, cuts, -0.22, 0.18) * values
    return jnp.clip(values, min=-bound, max=bound).astype(held_as)


def setup_inputs(seed: int = 0) -> dict:
    arg_keys = jax.random.split(jax.random.key(seed), 4)
    return {
        "voltages": normal_values(arg_keys[0], (2, FEEDS, SAMPLES), 1.0, 6.0, ((1, 8), (2, 4))),
        "usable": with_ends((jax.random.randint(arg_keys[1], (CHANNELS, FEEDS), 0, 8) < 7).astype(jnp.int32), jax.random.fold_in(arg_keys[1], 1), 0, 1),
        "auto_power": jnp.clip(jnp.exp(math.log(4.0) - 2.0794415 * jax.random.uniform(arg_keys[2], (CHANNELS, FEEDS), jnp.float32) ** levels(arg_keys[2], (CHANNELS, FEEDS), ((0, 32),), -0.2, 0.2)), 0.5, 4.0),
    }


def prototype(tap_count, channels):
    position = lax.iota(jnp.float32, tap_count * channels)
    offset = (position - 0.5 * tap_count * channels + 0.5) / channels
    window = 0.5 - 0.5 * jnp.cos(2.0 * jnp.pi * (position + 0.5) / (tap_count * channels))
    return (jnp.sin(jnp.pi * offset) / (jnp.pi * offset) * window).reshape(tap_count, channels)

def channelize(group_volts):
    samples = group_volts.astype(jnp.float32)
    count_here = samples.shape[1]
    leading = jnp.zeros((2, count_here, (TAPS - 1) * CHANNELS), jnp.float32)
    extended = jnp.concatenate([leading, samples], axis=2)
    extended = extended.reshape(2, count_here, SPECTRA + TAPS - 1, CHANNELS)
    coeffs = prototype(TAPS, CHANNELS)
    filtered = coeffs[0] * extended[:, :, 0:SPECTRA]
    for tap_index in range(1, TAPS):
        filtered = filtered + coeffs[tap_index] * extended[:, :, tap_index:tap_index + SPECTRA]
    spectrum = jnp.fft.fft(lax.complex(filtered[0], filtered[1]), axis=-1) / math.sqrt(CHANNELS)
    return jnp.stack([jnp.real(spectrum), jnp.imag(spectrum)]).astype(jnp.bfloat16)

def solve_group(pieces):
    spectra, usable, auto_power = pieces
    values = spectra.astype(jnp.float32)
    rotated = jnp.stack([values[:, 1], -values[:, 0]], axis=1)
    stacked = jnp.stack([values, rotated], axis=1)
    visibility = jnp.einsum('cqpit,cpjt->cqij', stacked, values, precision=lax.Precision.HIGHEST)
    weight = usable.astype(jnp.float32)
    diagonal = jnp.diagonal(visibility[:, 0], axis1=1, axis2=2)
    shifted = SPECTRA * auto_power - diagonal
    current = jnp.stack([weight, jnp.zeros_like(weight)], axis=1)
    result = current
    length = jnp.ones((weight.shape[0],), jnp.float32)
    for iteration in range(ITERS):
        masked = weight[:, None] * current
        product = jnp.einsum('cqij,cpj->cqpi', visibility, masked, precision=lax.Precision.HIGHEST)
        real_part = product[:, 0, 0] - product[:, 1, 1]
        imag_part = product[:, 0, 1] + product[:, 1, 0]
        result = weight[:, None] * (jnp.stack([real_part, imag_part], axis=1) + shifted[:, None] * masked)
        length = jnp.sqrt(lax.optimization_barrier(jnp.sum(result * result, axis=(1, 2))) + 1e-06)
        current = result / length[:, None, None]
    return result / jnp.sqrt(length)[:, None, None]

def reference(voltages, usable, auto_power):
    per_group = FEEDS // N_CHAN
    grouped = voltages.reshape(2, N_CHAN, per_group, SAMPLES).transpose(1, 0, 2, 3)
    spectra = lax.map(channelize, grouped)
    spectra = spectra.transpose(1, 0, 2, 3, 4).reshape(2, FEEDS, SPECTRA, CHANNELS)
    group_size = math.gcd(CHANNELS // (N_SECTION * N_CHAN), 8)
    group_count = CHANNELS // group_size
    ordered = spectra.reshape(2, FEEDS, SPECTRA, group_count, group_size).transpose(3, 4, 0, 1, 2)
    gains = lax.map(solve_group, (ordered, usable.reshape(group_count, group_size, FEEDS), auto_power.reshape(group_count, group_size, FEEDS)))
    return gains.reshape(CHANNELS, 2, FEEDS).transpose(1, 0, 2)
```

```python
import functools
import math

import jax
import jax.numpy as jnp
import numpy as np
from jax import lax
from jax.experimental import pallas as pl
from jax.experimental.pallas import tpu as pltpu
from jax.sharding import PartitionSpec as P

CHANNELS = 4096
TAPS = 4
ITERS = 5
LANES = 128
OUTER = CHANNELS // LANES
TILE = 16
epsilon = 1e-06
F32 = jnp.float32
BF16 = jnp.bfloat16
VMEM_LIMIT = 60 * 1024 * 1024


def prototype():
    position = np.arange(TAPS * CHANNELS, dtype=np.float64)
    offset = (position - 0.5 * TAPS * CHANNELS + 0.5) / CHANNELS
    window = 0.5 - 0.5 * np.cos(2.0 * np.pi * (position + 0.5) / (TAPS * CHANNELS))
    taps = np.sin(np.pi * offset) / (np.pi * offset) * window
    return taps.astype(np.float32).reshape(TAPS, OUTER, LANES)


def second_table():
    j = np.arange(LANES)
    twist = np.exp(-2j * np.pi * (np.outer(np.arange(OUTER), j) % CHANNELS) / CHANNELS)
    inner = np.exp(-2j * np.pi * (np.outer(j, j) % LANES) / LANES) / math.sqrt(CHANNELS)
    tr, ti = (jnp.asarray(a.astype(np.float32))[:, :, None] for a in (twist.real, twist.imag))
    fr, fi = (jnp.asarray(a.astype(np.float32))[None] for a in (inner.real, inner.imag))
    re, im = tr * fr - ti * fi, tr * fi + ti * fr
    table = jnp.concatenate(
        [jnp.concatenate([re, im], axis=2), jnp.concatenate([-im, re], axis=2)], axis=1
    )
    high = table.astype(BF16)
    low = (table - lax.optimization_barrier(high).astype(F32)).astype(BF16)
    return high, low


def times(z, w):
    zr, zi = z
    wr, wi = float(w.real), float(w.imag)
    if abs(wi) < 1e-12 and abs(wr - 1) < 1e-12:
        return zr, zi
    if abs(wr) < 1e-12 and abs(wi + 1) < 1e-12:
        return zi, -zr
    half = math.sqrt(0.5)
    if abs(wr - half) < 1e-12 and abs(wi + half) < 1e-12:
        return (zr + zi) * half, (zi - zr) * half
    if abs(wr + half) < 1e-12 and abs(wi + half) < 1e-12:
        return (zi - zr) * half, (zr + zi) * -half
    return zr * wr - zi * wi, zr * wi + zi * wr


def plus(a, b):
    return a[0] + b[0], a[1] + b[1]


def minus(a, b):
    return a[0] - b[0], a[1] - b[1]


def dft(values):
    n = len(values)
    if n == 1:
        return values
    even, odd = dft(values[0::2]), dft(values[1::2])
    odd = [times(z, np.exp(-2j * np.pi * k / n)) for k, z in enumerate(odd)]
    return [plus(a, b) for a, b in zip(even, odd)] + [minus(a, b) for a, b in zip(even, odd)]


QUICK = 8
SLOW = OUTER // QUICK


def channelize_kernel(lead, frames, x_ref, prev_ref, taps_ref, high_ref, low_ref, *rest):
    out_ref, filtered, quick, ah, al, bh, bl = rest[-7:]
    rows = frames * TILE

    def filter_step(m, carry):
        column = m * LANES
        taps = [taps_ref[t, pl.ds(m, 1), :] for t in range(TAPS)]
        for part in range(2):
            window = []
            for frame in range(1 - TAPS, frames):
                if frame < 0:
                    at = pl.multiple_of((lead + frame) * CHANNELS + column, LANES)
                    tile = prev_ref[part, :, pl.ds(at, LANES)]
                else:
                    at = pl.multiple_of(frame * CHANNELS + column, LANES)
                    tile = x_ref[part, :, pl.ds(at, LANES)]
                window.append(tile.astype(F32))
            for b in range(frames):
                total = window[b] * taps[0]
                for t in range(1, TAPS):
                    total = total + window[b + t] * taps[t]
                filtered[m, part, b * TILE : (b + 1) * TILE, :] = total
        return carry

    lax.fori_loop(0, OUTER, filter_step, 0)

    def quick_step(r, carry):
        at = pl.ds(pl.multiple_of(r * 8, 8), 8)
        for m0 in range(SLOW):
            values = [
                tuple(filtered[m1 * SLOW + m0, part, at, :] for part in range(2))
                for m1 in range(QUICK)
            ]
            for k, z in enumerate(dft(values)):
                z = times(z, np.exp(-2j * np.pi * m0 * k / OUTER))
                for part in range(2):
                    quick[k, m0, part, at, :] = z[part]
        return carry

    lax.fori_loop(0, rows // 8, quick_step, 0)

    def slow_step(k, hi_ref, lo_ref):
        for r in range(0, rows, TILE):
            at = slice(r, r + TILE)
            values = [
                tuple(quick[k, m0, part, at, :] for part in range(2)) for m0 in range(SLOW)
            ]
            for i, z in enumerate(dft(values)):
                for part in range(2):
                    hi = z[part].astype(BF16)
                    lo = (z[part] - hi.astype(F32)).astype(BF16)
                    hi_ref[i, at, part * LANES : (part + 1) * LANES] = hi
                    lo_ref[i, at, part * LANES : (part + 1) * LANES] = lo

    def matmul_step(k, hi_ref, lo_ref):
        for i in range(SLOW):
            k1 = i * QUICK + k
            hi, lo = hi_ref[i], lo_ref[i]
            th, tl = high_ref[k1], low_ref[k1]
            dot = functools.partial(jnp.dot, preferred_element_type=F32)
            res = (dot(hi, th) + dot(lo, th)) + dot(hi, tl)
            for part in range(2):
                piece = res[:, part * LANES : (part + 1) * LANES].astype(BF16)
                out_ref[k1, part, 0] = piece.reshape(frames, TILE, LANES)

    slow_step(0, ah, al)

    def pair_step(i, carry):
        k = 2 * i
        slow_step(k + 1, bh, bl)
        matmul_step(k, ah, al)
        slow_step(jnp.minimum(k + 2, QUICK - 1), ah, al)
        matmul_step(k + 1, bh, bl)
        return carry

    lax.fori_loop(0, QUICK // 2, pair_step, 0)


def channelize(voltages, before, high, low, earlier):
    feeds_here = voltages.shape[1]
    blocks = voltages.shape[2] // CHANNELS
    frames = 8
    first = 0 if before is not None else 1
    steps = 1 if before is not None else blocks // frames - 1
    lead = TAPS - 1 if before is not None else 4
    if before is None:
        before = voltages
    per = frames // 4
    if lead == 4:
        before_map = lambda f, b: (0, f, (b + first) * per - 1)
    else:
        before_map = lambda f, b: (0, f, 0)
    in_specs = [
        pl.BlockSpec((2, TILE, frames * CHANNELS), lambda f, b: (0, f, b + first)),
        pl.BlockSpec((2, TILE, lead * CHANNELS), before_map),
        pl.BlockSpec((TAPS, OUTER, LANES), lambda f, b: (0, 0, 0)),
        pl.BlockSpec((OUTER, 2 * LANES, 2 * LANES), lambda f, b: (0, 0, 0)),
        pl.BlockSpec((OUTER, 2 * LANES, 2 * LANES), lambda f, b: (0, 0, 0)),
    ]
    args = [voltages, before, jnp.asarray(prototype()), high, low]
    aliases = {}
    if earlier is not None:
        in_specs.append(pl.BlockSpec(memory_space=pl.ANY))
        args.append(earlier)
        aliases = {5: 0}
    rows = frames * TILE
    share = steps * frames * feeds_here
    return pl.pallas_call(
        functools.partial(channelize_kernel, lead, frames),
        grid=(feeds_here // TILE, steps),
        in_specs=in_specs,
        out_specs=pl.BlockSpec(
            (OUTER, 2, 1, frames, TILE, LANES), lambda f, b: (0, 0, f, b + first, 0, 0)
        ),
        out_shape=jax.ShapeDtypeStruct(
            (OUTER, 2, feeds_here // TILE, blocks, TILE, LANES), BF16
        ),
        scratch_shapes=[
            pltpu.VMEM((OUTER, 2, rows, LANES), F32),
            pltpu.VMEM((QUICK, SLOW, 2, rows, LANES), F32),
        ]
        + [pltpu.VMEM((SLOW, rows, 2 * LANES), BF16)] * 4,
        input_output_aliases=aliases,
        compiler_params=pltpu.CompilerParams(
            dimension_semantics=("arbitrary", "arbitrary"), vmem_limit_bytes=VMEM_LIMIT
        ),
        cost_estimate=pl.CostEstimate(
            flops=share * CHANNELS * 2 * 256 * 6,
            bytes_accessed=share * CHANNELS * 8,
            transcendentals=0,
        ),
    )(*args)


def fold_rows(parts):
    row = lax.broadcasted_iota(jnp.int32, (8, LANES), 0)
    half = []
    for i in range(4):
        a, b = parts[i], parts[i + 4]
        keep = jnp.where(row < 4, a, b)
        move = jnp.where(row < 4, b, a)
        half.append(keep + pltpu.roll(move, 4, 0))
    for shift in (2, 1):
        count = len(half) // 2
        bit = (row & shift) == 0
        half = [
            jnp.where(
                bit,
                half[i] + pltpu.roll(half[i], 8 - shift, 0),
                half[i + count] + pltpu.roll(half[i + count], shift, 0),
            )
            for i in range(count)
        ]
    return half[0]


def solve_kernel(sizes, *refs):
    n_section, n_chan, feeds, blocks, chunks, kc = sizes
    (spectra_hbm, weight_ref, power_ref, out_ref,
     spectra, diagonal, local_p, half_in, half_sum, piece_in, full_p, scaled,
     norm, local_q, q_in, y_ref,
     load_sem, half_ss, half_rs, piece_ss, piece_rs, gather_ss, gather_rs,
     share_ss, share_rs, norm_ss, norm_rs, q_ss, q_rs, y_ss, y_rs) = refs
    tiles = feeds // TILE
    n_z = n_chan // 2
    me_s = lax.axis_index("section")
    me_c = lax.axis_index("chan")
    core, z = me_c % 2, me_c // 2
    half_k = kc // 2
    half_rows = half_k * 2 * blocks
    piece_rows = half_rows // n_z
    k_piece = kc // n_section

    def remote(src, dst, ss, rs, **where):
        return pltpu.make_async_remote_copy(
            src_ref=src, dst_ref=dst, send_sem=ss, recv_sem=rs,
            device_id=where, device_id_type=pl.DeviceIdType.MESH,
        )

    def load(c):
        at = pl.ds(c * kc, kc)
        return pltpu.make_async_copy(spectra_hbm.at[at], spectra.at[at], load_sem.at[c])

    def half_copy(c):
        return remote(local_p.at[c, 1 - core], half_in.at[c], half_ss.at[c], half_rs.at[c],
                      chan=z * 2 + (1 - core))

    def norm_copies(c):
        return [
            remote(norm.at[c, 0], norm.at[c, d], norm_ss.at[c, d - 1], norm_rs.at[c, d - 1],
                   chan=(me_c + d) % n_chan)
            for d in range(1, n_chan)
        ]

    def piece_copies(c):
        copies = []
        for d in range(1, n_z):
            to = (z + d) % n_z
            rows = pl.ds(pl.multiple_of(to * piece_rows, piece_rows), piece_rows)
            copies.append(remote(half_sum.at[c, rows], piece_in.at[c, d - 1],
                                 piece_ss.at[c, d - 1], piece_rs.at[c, d - 1],
                                 chan=to * 2 + core))
        return copies

    def gather_copies(c, receive=False):
        copies = []
        for d in range(1, n_z):
            to = (z + d) % n_z
            owner = (z - d + n_z) % n_z if receive else z
            rows = pl.ds(pl.multiple_of(owner * piece_rows, piece_rows), piece_rows)
            view = full_p.at[c, core, rows]
            copies.append(remote(view, view, gather_ss.at[c, d - 1], gather_rs.at[c, d - 1],
                                 chan=to * 2 + core))
        return copies

    def share_copy(c, receive=False):
        view = full_p.at[c, 1 - core if receive else core]
        return remote(view, view, share_ss.at[c], share_rs.at[c], chan=z * 2 + (1 - core))

    def q_copies(c):
        copies = []
        for d in range(1, n_section):
            to = (me_s + d) % n_section
            copies.append(remote(local_q.at[c, pl.ds(to * k_piece, k_piece)], q_in.at[c, d - 1],
                                 q_ss.at[c, d - 1], q_rs.at[c, d - 1], section=to))
        return copies

    def y_copies(c, receive=False):
        copies = []
        for d in range(1, n_section):
            to = (me_s + d) % n_section
            owner = (me_s - d + n_section) % n_section if receive else me_s
            view = y_ref.at[c, pl.ds(owner * k_piece, k_piece)]
            copies.append(remote(view, view, y_ss.at[c, d - 1], y_rs.at[c, d - 1], section=to))
        return copies

    def pair(k1, tile, b):
        return spectra[k1, 0, tile, b].astype(F32), spectra[k1, 1, tile, b].astype(F32)

    def project(it, c):
        @pl.when(it == 0)
        def _():
            load(c).wait()

        @pl.when(it > 0)
        def _():
            for copy in y_copies(c):
                copy.wait_send()
            for copy in y_copies(c, receive=True):
                copy.wait_recv()

        def one(k, carry):
            k1 = c * kc + k
            yr = [y_ref[c, k, 0, t * TILE : (t + 1) * TILE, :].astype(F32) for t in range(tiles)]
            yi = [y_ref[c, k, 1, t * TILE : (t + 1) * TILE, :].astype(F32) for t in range(tiles)]
            square = sum(a * a for a in yr + yi)
            norm[c, 0, pl.ds(k, 1), :] = jnp.sum(square, axis=0, keepdims=True)

            def group(g, carry):
                rows_r, rows_i = [], []
                for s in range(8):
                    b = g * 8 + s
                    ar = ai = None
                    for t in range(tiles):
                        re, im = pair(k1, t, b)
                        pr = re * yr[t] + im * yi[t]
                        pi = re * yi[t] - im * yr[t]
                        ar = pr if ar is None else ar + pr
                        ai = pi if ai is None else ai + pi
                    rows_r.append(ar[:8] + ar[8:])
                    rows_i.append(ai[:8] + ai[8:])
                at = (k % half_k) * (2 * blocks) + g * 8
                h = k // half_k
                local_p[c, h, pl.ds(pl.multiple_of(at, 8), 8), :] = fold_rows(rows_r)
                at = at + blocks
                local_p[c, h, pl.ds(pl.multiple_of(at, 8), 8), :] = fold_rows(rows_i)
                return carry

            lax.fori_loop(0, blocks // 8, group, 0)
            return carry

        lax.fori_loop(0, kc, one, 0)
        half_copy(c).start()
        for copy in norm_copies(c):
            copy.start()

        @pl.when(it == 0)
        def _():
            def one_d(k, carry):
                k1 = c * kc + k

                def step(b, totals):
                    new = []
                    for t in range(tiles):
                        re, im = pair(k1, t, b)
                        new.append(totals[t] + (re * re + im * im))
                    return tuple(new)

                zero = jnp.zeros((TILE, LANES), F32)
                totals = lax.fori_loop(0, blocks, step, (zero,) * tiles)
                for t in range(tiles):
                    at = slice(t * TILE, (t + 1) * TILE)
                    diagonal[k1, at, :] = blocks * power_ref[k1, at, :] - totals[t]
                return carry

            lax.fori_loop(0, kc, one_d, 0)

    def add_half(it, c):
        half_copy(c).wait()
        half_sum[c] = local_p[c, core] + half_in[c]
        for copy in piece_copies(c):
            copy.start()

    def add_pieces(it, c):
        for copy in piece_copies(c):
            copy.wait()
        rows = pl.ds(pl.multiple_of(z * piece_rows, piece_rows), piece_rows)
        total = half_sum[c, rows, :]
        for d in range(1, n_z):
            total = total + piece_in[c, d - 1]
        full_p[c, core, rows, :] = total
        for copy in gather_copies(c):
            copy.start()

    def share_half(it, c):
        for copy in gather_copies(c):
            copy.wait_send()
        for copy in gather_copies(c, receive=True):
            copy.wait_recv()
        share_copy(c).start()

    def expand(it, c):
        share_copy(c).wait_send()
        share_copy(c, receive=True).wait_recv()
        for copy in norm_copies(c):
            copy.wait()
        length = norm[c, 0]
        for d in range(1, n_chan):
            length = length + norm[c, d]
        inverse = jnp.where(it == 0, 1.0, 1.0 / jnp.sqrt(length + epsilon))
        norm_scale = scaled.at[pl.ds(2 * blocks, 8)]
        norm_scale[...] = inverse

        def one(k, carry):
            k1 = c * kc + k
            inv = scaled[pl.ds(2 * blocks + k, 1), :]
            at = pl.multiple_of((k % half_k) * (2 * blocks), 2 * blocks)
            scaled[0 : 2 * blocks, :] = full_p[c, k // half_k, pl.ds(at, 2 * blocks), :] * inv

            def group(g, totals):
                totals = list(totals)
                for s in range(4):
                    b = g * 4 + s
                    pr = scaled[pl.ds(b, 1), :]
                    pi = scaled[pl.ds(blocks + b, 1), :]
                    for t in range(tiles):
                        re, im = pair(k1, t, b)
                        totals[2 * t] = totals[2 * t] + (re * pr - im * pi)
                        totals[2 * t + 1] = totals[2 * t + 1] + (re * pi + im * pr)
                return tuple(totals)

            zero = jnp.zeros((TILE, LANES), F32)
            totals = lax.fori_loop(0, blocks // 4, group, (zero,) * (2 * tiles))
            for t in range(tiles):
                at = slice(t * TILE, (t + 1) * TILE)
                weight = weight_ref[k1, at, :]
                shift = diagonal[k1, at, :] * inv
                for part in range(2):
                    now = y_ref[c, k, part, at, :].astype(F32)
                    value = weight * (totals[2 * t + part] + shift * now)
                    local_q[c, k, part, at, :] = value.astype(BF16)
            return carry

        lax.fori_loop(0, kc, one, 0)
        for copy in q_copies(c):
            copy.start()

    def add_sections(it, c):
        for copy in q_copies(c):
            copy.wait()
        for k in range(k_piece):
            for part in range(2):
                at = me_s * k_piece + k
                total = local_q[c, at, part].astype(F32)
                for d in range(1, n_section):
                    total = total + q_in[c, d - 1, k, part].astype(F32)
                y_ref[c, at, part] = total.astype(BF16)
        for copy in y_copies(c):
            copy.start()

    barrier = pltpu.get_barrier_semaphore()
    for d in range(1, n_chan):
        pl.semaphore_signal(barrier, inc=1, device_id={"chan": (me_c + d) % n_chan},
                            device_id_type=pl.DeviceIdType.MESH)
    for d in range(1, n_section):
        pl.semaphore_signal(barrier, inc=1, device_id={"section": (me_s + d) % n_section},
                            device_id_type=pl.DeviceIdType.MESH)

    @pl.loop(0, chunks)
    def _(c):
        load(c).start()

    @pl.loop(0, chunks)
    def _(c):
        for k in range(kc):
            y_ref[c, k, 0] = weight_ref[c * kc + k].astype(BF16)
            y_ref[c, k, 1] = jnp.zeros((feeds, LANES), BF16)
        norm[c, 0] = jnp.zeros((8, LANES), F32)

    pl.semaphore_wait(barrier, n_chan + n_section - 2)

    stages = [project, add_half, add_pieces, share_half, expand, add_sections]
    period = max(chunks, len(stages) + 1)

    @pl.loop(0, ITERS * period + len(stages))
    def _(slot):
        for lag, stage in reversed(list(enumerate(stages))):
            turn = slot - lag + period
            it, c = turn // period - 1, turn % period

            @pl.when((it >= 0) & (it < ITERS) & (c < chunks))
            def _():
                stage(it, c)

    @pl.loop(0, chunks)
    def _(c):
        for copy in y_copies(c):
            copy.wait_send()
        for copy in y_copies(c, receive=True):
            copy.wait_recv()

    out_ref[...] = y_ref[...]


def solve(spectra, weight, power, n_section, n_chan):
    feeds, blocks = spectra.shape[2] * TILE, spectra.shape[3]
    kc = n_section
    chunks = OUTER // kc
    n_z = n_chan // 2
    half_rows = kc * blocks
    piece_rows = half_rows // n_z
    k_piece = kc // n_section
    dma = pltpu.SemaphoreType.DMA
    per = lambda n: dma((chunks, n))
    scratch = [
        pltpu.VMEM(spectra.shape, BF16),
        pltpu.VMEM((OUTER, feeds, LANES), F32),
        pltpu.VMEM((chunks, 2, half_rows, LANES), F32),
        pltpu.VMEM((chunks, half_rows, LANES), F32),
        pltpu.VMEM((chunks, half_rows, LANES), F32),
        pltpu.VMEM((chunks, n_z - 1, piece_rows, LANES), F32),
        pltpu.VMEM((chunks, 2, half_rows, LANES), F32),
        pltpu.VMEM((2 * blocks + 8, LANES), F32),
        pltpu.VMEM((chunks, n_chan, 8, LANES), F32),
        pltpu.VMEM((chunks, kc, 2, feeds, LANES), BF16),
        pltpu.VMEM((chunks, n_section - 1, k_piece, 2, feeds, LANES), BF16),
        pltpu.VMEM((chunks, kc, 2, feeds, LANES), BF16),
        dma((chunks,)),
        dma((chunks,)), dma((chunks,)),
        per(n_z - 1), per(n_z - 1), per(n_z - 1), per(n_z - 1),
        dma((chunks,)), dma((chunks,)),
        per(n_chan - 1), per(n_chan - 1),
        per(n_section - 1), per(n_section - 1), per(n_section - 1), per(n_section - 1),
    ]
    vmem = pl.BlockSpec(memory_space=pltpu.VMEM)
    return pl.pallas_call(
        functools.partial(solve_kernel, (n_section, n_chan, feeds, blocks, chunks, kc)),
        in_specs=[pl.BlockSpec(memory_space=pl.ANY), vmem, vmem],
        out_specs=vmem,
        out_shape=jax.ShapeDtypeStruct((chunks, kc, 2, feeds, LANES), BF16),
        scratch_shapes=scratch,
        compiler_params=pltpu.CompilerParams(
            collective_id=1, has_side_effects=True, vmem_limit_bytes=VMEM_LIMIT
        ),
    )(spectra, weight, power)


def local(voltages, usable, auto_power):
    n_section, n_chan = lax.axis_size("section"), lax.axis_size("chan")
    margin = (TAPS - 1) * CHANNELS
    tail = voltages[:, :, voltages.shape[2] - margin :]
    history = lax.ppermute(tail, "section", [(i, i + 1) for i in range(n_section - 1)])

    small = jnp.stack([usable.astype(F32), auto_power], axis=0)
    small = lax.all_to_all(small, "chan", split_axis=2, concat_axis=1, tiled=True)
    small = lax.all_gather(small, "section", axis=1, tiled=True)
    feeds_here = small.shape[2]
    small = small.reshape(2, LANES, OUTER, feeds_here).transpose(0, 2, 3, 1)

    high, low = second_table()
    spectra = channelize(voltages, None, high, low, None)
    spectra = channelize(voltages, history, high, low, spectra)

    result = solve(spectra, small[0], small[1], n_section, n_chan)
    result = result.reshape(OUTER, 2, feeds_here, LANES)
    width = LANES // n_section
    result = lax.dynamic_slice_in_dim(result, lax.axis_index("section") * width, width, axis=3)
    result = result.transpose(1, 3, 0, 2).reshape(2, width * OUTER, feeds_here)
    result = lax.all_to_all(result, "chan", split_axis=1, concat_axis=2, tiled=True)
    result = result.astype(F32)
    length = jnp.sqrt(jnp.sum(result * result, axis=(0, 2)) + epsilon)
    return result / jnp.sqrt(length)[None, :, None]


def solution(mesh):
    in_specs = (
        P(None, "chan", "section"),
        P(("section", "chan"), None),
        P(("section", "chan"), None),
    )
    out_specs = P(None, ("section", "chan"), None)
    return jax.shard_map(local, mesh=mesh, in_specs=in_specs, out_specs=out_specs, check_vma=False)
```

```python
import functools
import math

import jax
import jax.numpy as jnp
import numpy as np
from jax import lax
from jax.experimental import pallas as pl
from jax.experimental.pallas import tpu as pltpu
from jax.sharding import PartitionSpec as P

CHANNELS = 4096
TAPS = 4
ITERS = 5
LANES = 128
OUTER = CHANNELS // LANES
TILE = 16
epsilon = 1e-06
F32 = jnp.float32
BF16 = jnp.bfloat16
VMEM_LIMIT = 60 * 1024 * 1024


def prototype():
    position = np.arange(TAPS * CHANNELS, dtype=np.float64)
    offset = (position - 0.5 * TAPS * CHANNELS + 0.5) / CHANNELS
    window = 0.5 - 0.5 * np.cos(2.0 * np.pi * (position + 0.5) / (TAPS * CHANNELS))
    taps = np.sin(np.pi * offset) / (np.pi * offset) * window
    return taps.astype(np.float32).reshape(TAPS, OUTER, LANES)


def table_seed():
    j = np.arange(LANES)
    inner = np.exp(-2j * np.pi * (np.outer(j, j) % LANES) / LANES) / math.sqrt(CHANNELS)
    twist = np.exp(-2j * np.pi * np.repeat(j[:, None], LANES, axis=1) / CHANNELS)
    parts = np.stack([inner.real, inner.imag, twist.real, twist.imag])
    return jnp.asarray(parts.astype(np.float32))


def times(z, w):
    zr, zi = z
    wr, wi = float(w.real), float(w.imag)
    if abs(wi) < 1e-12 and abs(wr - 1) < 1e-12:
        return zr, zi
    if abs(wr) < 1e-12 and abs(wi + 1) < 1e-12:
        return zi, -zr
    half = math.sqrt(0.5)
    if abs(wr - half) < 1e-12 and abs(wi + half) < 1e-12:
        return (zr + zi) * half, (zi - zr) * half
    if abs(wr + half) < 1e-12 and abs(wi + half) < 1e-12:
        return (zi - zr) * half, (zr + zi) * -half
    return zr * wr - zi * wi, zr * wi + zi * wr


def plus(a, b):
    return a[0] + b[0], a[1] + b[1]


def minus(a, b):
    return a[0] - b[0], a[1] - b[1]


def dft(values):
    n = len(values)
    if n == 1:
        return values
    even, odd = dft(values[0::2]), dft(values[1::2])
    odd = [times(z, np.exp(-2j * np.pi * k / n)) for k, z in enumerate(odd)]
    return [plus(a, b) for a, b in zip(even, odd)] + [minus(a, b) for a, b in zip(even, odd)]


QUICK = 8
SLOW = OUTER // QUICK


def channelize_kernel(sizes, *refs):
    frames, tiles, early, n_section = sizes
    (x_ref, prev_ref, taps_ref, seed_ref, whole_ref, out_ref,
     filtered, quick, ah, al, bh, bl, high, low, turning, history, send_sem, recv_sem) = refs
    rows = frames * TILE
    margin = (TAPS - 1) * CHANNELS
    step = pl.program_id(0)
    last = pl.num_programs(0) - 1
    me = lax.axis_index("section")

    def history_copy(tile):
        start = whole_ref.shape[2] - margin
        src = whole_ref.at[:, pl.ds(tile * TILE, TILE), pl.ds(start, margin)]
        return pltpu.make_async_remote_copy(
            src_ref=src, dst_ref=history.at[tile], send_sem=send_sem.at[tile],
            recv_sem=recv_sem.at[tile], device_id={"section": (me + 1) % n_section},
            device_id_type=pl.DeviceIdType.MESH,
        )

    @pl.when(step == 0)
    def _():
        barrier = pltpu.get_barrier_semaphore()
        for to in ((me + 1) % n_section, (me + n_section - 1) % n_section):
            pl.semaphore_signal(barrier, inc=1, device_id={"section": to},
                                device_id_type=pl.DeviceIdType.MESH)
        pl.semaphore_wait(barrier, 2)

        @pl.when(me < n_section - 1)
        def _():
            for tile in range(tiles):
                history_copy(tile).start()

        @pl.when(me == 0)
        def _():
            def clear(i, carry):
                at = pl.ds(pl.multiple_of(i * LANES, LANES), LANES)
                for tile in range(tiles):
                    for part in range(2):
                        history[tile, part, :, at] = jnp.zeros((TILE, LANES), BF16)
                return carry

            lax.fori_loop(0, margin // LANES, clear, 0)

        turning[...] = seed_ref[0:2]

        def build(k1, carry):
            for r in range(0, LANES, TILE):
                at = slice(r, r + TILE)
                below = slice(LANES + r, LANES + r + TILE)
                re, im = turning[0, at, :], turning[1, at, :]
                for rows_at, left, value in ((at, 0, re), (at, LANES, im),
                                             (below, 0, -im), (below, LANES, re)):
                    top = value.astype(BF16)
                    columns = slice(left, left + LANES)
                    high[k1, rows_at, columns] = top
                    low[k1, rows_at, columns] = (value - top.astype(F32)).astype(BF16)
                tr, ti = seed_ref[2, at, :], seed_ref[3, at, :]
                turning[0, at, :] = re * tr - im * ti
                turning[1, at, :] = re * ti + im * tr
            return carry

        lax.fori_loop(0, OUTER, build, 0)

    def run_filter(before):
        def filter_step(m, carry):
            column = m * LANES
            taps = [taps_ref[t, pl.ds(m, 1), :] for t in range(TAPS)]
            for part in range(2):
                window = []
                for frame in range(1 - TAPS, frames):
                    if frame < 0:
                        tile = before(frame, part, column)
                    else:
                        at = pl.multiple_of(frame * CHANNELS + column, LANES)
                        tile = x_ref[part, :, pl.ds(at, LANES)]
                    window.append(tile.astype(F32))
                for b in range(frames):
                    total = window[b] * taps[0]
                    for t in range(1, TAPS):
                        total = total + window[b + t] * taps[t]
                    filtered[m, part, b * TILE : (b + 1) * TILE, :] = total
            return carry

        lax.fori_loop(0, OUTER, filter_step, 0)

    @pl.when(step < early)
    def _():
        def before(frame, part, column):
            at = pl.multiple_of((4 + frame) * CHANNELS + column, LANES)
            return prev_ref[part, :, pl.ds(at, LANES)]

        run_filter(before)

    @pl.when(step >= early)
    def _():
        tile = step - early

        @pl.when(me > 0)
        def _():
            history_copy(tile).wait_recv()

        def before(frame, part, column):
            at = pl.multiple_of((TAPS - 1 + frame) * CHANNELS + column, LANES)
            return history[tile, part, :, pl.ds(at, LANES)]

        run_filter(before)

    def quick_step(r, carry):
        at = pl.ds(pl.multiple_of(r * 8, 8), 8)
        for m0 in range(SLOW):
            values = [
                tuple(filtered[m1 * SLOW + m0, part, at, :] for part in range(2))
                for m1 in range(QUICK)
            ]
            for k, z in enumerate(dft(values)):
                z = times(z, np.exp(-2j * np.pi * m0 * k / OUTER))
                for part in range(2):
                    quick[k, m0, part, at, :] = z[part]
        return carry

    lax.fori_loop(0, rows // 8, quick_step, 0)

    def slow_step(k, hi_ref, lo_ref):
        for r in range(0, rows, TILE):
            at = slice(r, r + TILE)
            values = [
                tuple(quick[k, m0, part, at, :] for part in range(2)) for m0 in range(SLOW)
            ]
            for i, z in enumerate(dft(values)):
                for part in range(2):
                    hi = z[part].astype(BF16)
                    lo = (z[part] - hi.astype(F32)).astype(BF16)
                    hi_ref[i, part, at, :] = hi
                    lo_ref[i, part, at, :] = lo

    def matmul_step(k, hi_ref, lo_ref):
        for i in range(SLOW):
            k1 = i * QUICK + k
            hi = jnp.concatenate([hi_ref[i, 0], hi_ref[i, 1]], axis=1)
            lo = jnp.concatenate([lo_ref[i, 0], lo_ref[i, 1]], axis=1)
            th, tl = high[k1], low[k1]
            dot = functools.partial(jnp.dot, preferred_element_type=F32)
            res = (dot(hi, th) + dot(lo, th)) + dot(hi, tl)
            for part in range(2):
                piece = res[:, part * LANES : (part + 1) * LANES].astype(BF16)
                out_ref[k1, part, 0] = piece.reshape(frames, TILE, LANES)

    slow_step(0, ah, al)

    def pair_step(i, carry):
        k = 2 * i
        slow_step(k + 1, bh, bl)
        matmul_step(k, ah, al)
        slow_step(jnp.minimum(k + 2, QUICK - 1), ah, al)
        matmul_step(k + 1, bh, bl)
        return carry

    lax.fori_loop(0, QUICK // 2, pair_step, 0)

    @pl.when((step == last) & (me < n_section - 1))
    def _():
        for tile in range(tiles):
            history_copy(tile).wait_send()


def channelize(voltages, n_section):
    feeds_here = voltages.shape[1]
    blocks = voltages.shape[2] // CHANNELS
    frames = 8
    tiles, groups = feeds_here // TILE, blocks // frames
    early = tiles * (groups - 1)
    rows = frames * TILE
    per = frames // 4

    def place(i):
        late = i >= early
        tile = jnp.where(late, i - early, i // (groups - 1))
        return tile, jnp.where(late, 0, 1 + i % (groups - 1))

    def x_map(i):
        tile, group = place(i)
        return 0, tile, group

    def prev_map(i):
        tile, group = place(jnp.minimum(i, early - 1))
        return 0, tile, group * per - 1

    def out_map(i):
        tile, group = place(i)
        return 0, 0, tile, group, 0, 0

    table = pltpu.VMEM((OUTER, 2 * LANES, 2 * LANES), BF16)
    half = pltpu.VMEM((SLOW, 2, rows, LANES), BF16)
    return pl.pallas_call(
        functools.partial(channelize_kernel, (frames, tiles, early, n_section)),
        grid=(tiles * groups,),
        in_specs=[
            pl.BlockSpec((2, TILE, frames * CHANNELS), x_map),
            pl.BlockSpec((2, TILE, 4 * CHANNELS), prev_map),
            pl.BlockSpec((TAPS, OUTER, LANES), lambda i: (0, 0, 0)),
            pl.BlockSpec((4, LANES, LANES), lambda i: (0, 0, 0)),
            pl.BlockSpec(memory_space=pl.ANY),
        ],
        out_specs=pl.BlockSpec((OUTER, 2, 1, frames, TILE, LANES), out_map),
        out_shape=jax.ShapeDtypeStruct((OUTER, 2, tiles, blocks, TILE, LANES), BF16),
        scratch_shapes=[
            pltpu.VMEM((OUTER, 2, rows, LANES), F32),
            pltpu.VMEM((QUICK, SLOW, 2, rows, LANES), F32),
            half, half, half, half, table, table,
            pltpu.VMEM((2, LANES, LANES), F32),
            pltpu.VMEM((tiles, 2, TILE, (TAPS - 1) * CHANNELS), BF16),
            pltpu.SemaphoreType.DMA((tiles,)),
            pltpu.SemaphoreType.DMA((tiles,)),
        ],
        compiler_params=pltpu.CompilerParams(
            dimension_semantics=("arbitrary",), vmem_limit_bytes=VMEM_LIMIT,
            collective_id=0, has_side_effects=True,
        ),
    )(voltages, voltages, jnp.asarray(prototype()), table_seed(), voltages)


def fold_rows(parts):
    row = lax.broadcasted_iota(jnp.int32, (8, LANES), 0)
    half = []
    for i in range(4):
        a, b = parts[i], parts[i + 4]
        keep = jnp.where(row < 4, a, b)
        move = jnp.where(row < 4, b, a)
        half.append(keep + pltpu.roll(move, 4, 0))
    for shift in (2, 1):
        count = len(half) // 2
        bit = (row & shift) == 0
        half = [
            jnp.where(
                bit,
                half[i] + pltpu.roll(half[i], 8 - shift, 0),
                half[i + count] + pltpu.roll(half[i + count], shift, 0),
            )
            for i in range(count)
        ]
    return half[0]


def solve_kernel(sizes, *refs):
    n_section, n_chan, feeds, blocks, chunks, kc = sizes
    (spectra_hbm, power_ref, out_ref,
     spectra, diagonal, local_p, half_in, half_sum, piece_in, full_p, scaled,
     norm, local_q, q_in, y_ref,
     load_sem, half_ss, half_rs, piece_ss, piece_rs, gather_ss, gather_rs,
     share_ss, share_rs, norm_ss, norm_rs, q_ss, q_rs, y_ss, y_rs) = refs
    tiles = feeds // TILE
    n_z = n_chan // 2
    me_s = lax.axis_index("section")
    me_c = lax.axis_index("chan")
    core, z = me_c % 2, me_c // 2
    half_k = kc // 2
    half_rows = half_k * 2 * blocks
    piece_rows = half_rows // n_z
    k_piece = kc // n_section

    def remote(src, dst, ss, rs, **where):
        return pltpu.make_async_remote_copy(
            src_ref=src, dst_ref=dst, send_sem=ss, recv_sem=rs,
            device_id=where, device_id_type=pl.DeviceIdType.MESH,
        )

    def load(c):
        at = pl.ds(c * kc, kc)
        return pltpu.make_async_copy(spectra_hbm.at[at], spectra.at[at], load_sem.at[c])

    def half_copy(c):
        return remote(local_p.at[c, 1 - core], half_in.at[c], half_ss.at[c], half_rs.at[c],
                      chan=z * 2 + (1 - core))

    def norm_copies(c):
        return [
            remote(norm.at[c, 0], norm.at[c, d], norm_ss.at[c, d - 1], norm_rs.at[c, d - 1],
                   chan=(me_c + d) % n_chan)
            for d in range(1, n_chan)
        ]

    def piece_copies(c):
        copies = []
        for d in range(1, n_z):
            to = (z + d) % n_z
            rows = pl.ds(pl.multiple_of(to * piece_rows, piece_rows), piece_rows)
            copies.append(remote(half_sum.at[c, rows], piece_in.at[c, d - 1],
                                 piece_ss.at[c, d - 1], piece_rs.at[c, d - 1],
                                 chan=to * 2 + core))
        return copies

    def gather_copies(c, receive=False):
        copies = []
        for d in range(1, n_z):
            to = (z + d) % n_z
            owner = (z - d + n_z) % n_z if receive else z
            rows = pl.ds(pl.multiple_of(owner * piece_rows, piece_rows), piece_rows)
            view = full_p.at[c, core, rows]
            copies.append(remote(view, view, gather_ss.at[c, d - 1], gather_rs.at[c, d - 1],
                                 chan=to * 2 + core))
        return copies

    def share_copy(c, receive=False):
        view = full_p.at[c, 1 - core if receive else core]
        return remote(view, view, share_ss.at[c], share_rs.at[c], chan=z * 2 + (1 - core))

    def q_copies(c):
        copies = []
        for d in range(1, n_section):
            to = (me_s + d) % n_section
            copies.append(remote(local_q.at[c, pl.ds(to * k_piece, k_piece)], q_in.at[c, d - 1],
                                 q_ss.at[c, d - 1], q_rs.at[c, d - 1], section=to))
        return copies

    def y_copies(c, receive=False):
        copies = []
        for d in range(1, n_section):
            to = (me_s + d) % n_section
            owner = (me_s - d + n_section) % n_section if receive else me_s
            view = y_ref.at[c, pl.ds(owner * k_piece, k_piece)]
            copies.append(remote(view, view, y_ss.at[c, d - 1], y_rs.at[c, d - 1], section=to))
        return copies

    def pair(k1, tile, b):
        return spectra[k1, 0, tile, b].astype(F32), spectra[k1, 1, tile, b].astype(F32)

    def store_rows(c, k, g, rows_r, rows_i):
        at = (k % half_k) * (2 * blocks) + g * 8
        h = k // half_k
        local_p[c, h, pl.ds(pl.multiple_of(at, 8), 8), :] = fold_rows(rows_r)
        at = at + blocks
        local_p[c, h, pl.ds(pl.multiple_of(at, 8), 8), :] = fold_rows(rows_i)

    def project(it, c):
        @pl.when(it == 0)
        def _():
            load(c).wait()

            def one(k, carry):
                k1 = c * kc + k
                power = [power_ref[k1, t * TILE : (t + 1) * TILE, :].astype(F32)
                         for t in range(tiles)]
                weight = [jnp.where(p > 0, 1.0, 0.0) for p in power]

                def group(g, totals):
                    totals = list(totals)
                    rows_r, rows_i = [], []
                    for s in range(8):
                        b = g * 8 + s
                        ar = ai = jnp.zeros((TILE, LANES), F32)
                        for t in range(tiles):
                            re, im = pair(k1, t, b)
                            ar = ar + re * weight[t]
                            ai = ai - im * weight[t]
                            totals[t] = totals[t] + (re * re + im * im)
                        rows_r.append(ar[:8] + ar[8:])
                        rows_i.append(ai[:8] + ai[8:])
                    store_rows(c, k, g, rows_r, rows_i)
                    return tuple(totals)

                zero = jnp.zeros((TILE, LANES), F32)
                totals = lax.fori_loop(0, blocks // 8, group, (zero,) * tiles)
                for t in range(tiles):
                    at = slice(t * TILE, (t + 1) * TILE)
                    diagonal[k1, at, :] = blocks * power[t] - totals[t]
                return carry

            lax.fori_loop(0, kc, one, 0)

        @pl.when(it > 0)
        def _():
            for copy in y_copies(c):
                copy.wait_send()
            for copy in y_copies(c, receive=True):
                copy.wait_recv()

            def one(k, carry):
                k1 = c * kc + k
                yr, yi = ([y_ref[c, k, part, t * TILE : (t + 1) * TILE, :].astype(F32)
                           for t in range(tiles)] for part in range(2))
                square = sum(a * a for a in yr + yi)
                norm[c, 0, pl.ds(k, 1), :] = jnp.sum(square, axis=0, keepdims=True)

                def group(g, carry):
                    rows_r, rows_i = [], []
                    for s in range(8):
                        b = g * 8 + s
                        ar = ai = None
                        for t in range(tiles):
                            re, im = pair(k1, t, b)
                            pr = re * yr[t] + im * yi[t]
                            pi = re * yi[t] - im * yr[t]
                            ar = pr if ar is None else ar + pr
                            ai = pi if ai is None else ai + pi
                        rows_r.append(ar[:8] + ar[8:])
                        rows_i.append(ai[:8] + ai[8:])
                    store_rows(c, k, g, rows_r, rows_i)
                    return carry

                lax.fori_loop(0, blocks // 8, group, 0)
                return carry

            lax.fori_loop(0, kc, one, 0)

        half_copy(c).start()
        for copy in norm_copies(c):
            copy.start()

    def add_half(it, c):
        half_copy(c).wait()
        half_sum[c] = local_p[c, core] + half_in[c]
        for copy in piece_copies(c):
            copy.start()

    def add_pieces(it, c):
        for copy in piece_copies(c):
            copy.wait()
        rows = pl.ds(pl.multiple_of(z * piece_rows, piece_rows), piece_rows)
        total = half_sum[c, rows, :]
        for d in range(1, n_z):
            total = total + piece_in[c, d - 1]
        full_p[c, core, rows, :] = total
        for copy in gather_copies(c):
            copy.start()

    def share_half(it, c):
        for copy in gather_copies(c):
            copy.wait_send()
        for copy in gather_copies(c, receive=True):
            copy.wait_recv()
        share_copy(c).start()

    def expand(it, c):
        share_copy(c).wait_send()
        share_copy(c, receive=True).wait_recv()
        for copy in norm_copies(c):
            copy.wait()
        length = norm[c, 0]
        for d in range(1, n_chan):
            length = length + norm[c, d]
        inverse = jnp.where(it == 0, 1.0, 1.0 / jnp.sqrt(length + epsilon))
        norm_scale = scaled.at[pl.ds(2 * blocks, 8)]
        norm_scale[...] = inverse

        def one(k, carry):
            k1 = c * kc + k
            inv = scaled[pl.ds(2 * blocks + k, 1), :]
            at = pl.multiple_of((k % half_k) * (2 * blocks), 2 * blocks)
            scaled[0 : 2 * blocks, :] = full_p[c, k // half_k, pl.ds(at, 2 * blocks), :] * inv

            def group(g, totals):
                totals = list(totals)
                for s in range(8):
                    b = g * 8 + s
                    pr = scaled[pl.ds(b, 1), :]
                    pi = scaled[pl.ds(blocks + b, 1), :]
                    for t in range(tiles):
                        re, im = pair(k1, t, b)
                        totals[2 * t] = totals[2 * t] + (re * pr - im * pi)
                        totals[2 * t + 1] = totals[2 * t + 1] + (re * pi + im * pr)
                return tuple(totals)

            zero = jnp.zeros((TILE, LANES), F32)
            totals = lax.fori_loop(0, blocks // 8, group, (zero,) * (2 * tiles))
            for t in range(tiles):
                at = slice(t * TILE, (t + 1) * TILE)
                usable = power_ref[k1, at, :].astype(F32) > 0
                shift = diagonal[k1, at, :] * inv
                for part in range(2):
                    now = y_ref[c, k, part, at, :].astype(F32)
                    value = jnp.where(usable, totals[2 * t + part] + shift * now, 0.0)
                    local_q[c, k, part, at, :] = value.astype(BF16)
            return carry

        lax.fori_loop(0, kc, one, 0)
        for copy in q_copies(c):
            copy.start()

    def add_sections(it, c):
        for copy in q_copies(c):
            copy.wait()
        for k in range(k_piece):
            for part in range(2):
                at = me_s * k_piece + k
                total = local_q[c, at, part].astype(F32)
                for d in range(1, n_section):
                    total = total + q_in[c, d - 1, k, part].astype(F32)
                y_ref[c, at, part] = total.astype(BF16)
        for copy in y_copies(c):
            copy.start()

    barrier = pltpu.get_barrier_semaphore()
    for d in range(1, n_chan):
        pl.semaphore_signal(barrier, inc=1, device_id={"chan": (me_c + d) % n_chan},
                            device_id_type=pl.DeviceIdType.MESH)
    for d in range(1, n_section):
        pl.semaphore_signal(barrier, inc=1, device_id={"section": (me_s + d) % n_section},
                            device_id_type=pl.DeviceIdType.MESH)

    @pl.loop(0, chunks)
    def _(c):
        load(c).start()

    @pl.loop(0, chunks)
    def _(c):
        for k in range(kc):
            power = power_ref[c * kc + k].astype(F32)
            y_ref[c, k, 0] = jnp.where(power > 0, 1.0, 0.0).astype(BF16)
            y_ref[c, k, 1] = jnp.zeros((feeds, LANES), BF16)
        norm[c, 0] = jnp.zeros((8, LANES), F32)

    pl.semaphore_wait(barrier, n_chan + n_section - 2)

    stages = [(7, add_sections), (3, add_pieces), (5, expand), (4, share_half), (1, add_half),
              (0, project)]
    span = 7
    period = max(chunks, span + 1)

    @pl.loop(0, ITERS * period + span)
    def _(slot):
        for lag, stage in stages:
            turn = slot - lag + period
            it, c = turn // period - 1, turn % period

            @pl.when((it >= 0) & (it < ITERS) & (c < chunks))
            def _():
                stage(it, c)

    @pl.loop(0, chunks)
    def _(c):
        for copy in y_copies(c):
            copy.wait_send()
        for copy in y_copies(c, receive=True):
            copy.wait_recv()

    out_ref[...] = y_ref[...]


def solve(spectra, power, n_section, n_chan):
    feeds, blocks = spectra.shape[2] * TILE, spectra.shape[3]
    kc = n_section
    chunks = OUTER // kc
    n_z = n_chan // 2
    half_rows = kc * blocks
    piece_rows = half_rows // n_z
    k_piece = kc // n_section
    dma = pltpu.SemaphoreType.DMA
    per = lambda n: dma((chunks, n))
    scratch = [
        pltpu.VMEM(spectra.shape, BF16),
        pltpu.VMEM((OUTER, feeds, LANES), F32),
        pltpu.VMEM((chunks, 2, half_rows, LANES), F32),
        pltpu.VMEM((chunks, half_rows, LANES), F32),
        pltpu.VMEM((chunks, half_rows, LANES), F32),
        pltpu.VMEM((chunks, n_z - 1, piece_rows, LANES), F32),
        pltpu.VMEM((chunks, 2, half_rows, LANES), F32),
        pltpu.VMEM((2 * blocks + 8, LANES), F32),
        pltpu.VMEM((chunks, n_chan, 8, LANES), F32),
        pltpu.VMEM((chunks, kc, 2, feeds, LANES), BF16),
        pltpu.VMEM((chunks, n_section - 1, k_piece, 2, feeds, LANES), BF16),
        pltpu.VMEM((chunks, kc, 2, feeds, LANES), BF16),
        dma((chunks,)),
        dma((chunks,)), dma((chunks,)),
        per(n_z - 1), per(n_z - 1), per(n_z - 1), per(n_z - 1),
        dma((chunks,)), dma((chunks,)),
        per(n_chan - 1), per(n_chan - 1),
        per(n_section - 1), per(n_section - 1), per(n_section - 1), per(n_section - 1),
    ]
    vmem = pl.BlockSpec(memory_space=pltpu.VMEM)
    return pl.pallas_call(
        functools.partial(solve_kernel, (n_section, n_chan, feeds, blocks, chunks, kc)),
        in_specs=[pl.BlockSpec(memory_space=pl.ANY), vmem],
        out_specs=vmem,
        out_shape=jax.ShapeDtypeStruct((chunks, kc, 2, feeds, LANES), BF16),
        scratch_shapes=scratch,
        compiler_params=pltpu.CompilerParams(
            collective_id=1, has_side_effects=True, vmem_limit_bytes=VMEM_LIMIT
        ),
    )(spectra, power)


def local(voltages, usable, auto_power):
    n_section, n_chan = lax.axis_size("section"), lax.axis_size("chan")
    power = (usable.astype(F32) * auto_power).astype(BF16)
    power = lax.all_to_all(power, "chan", split_axis=1, concat_axis=0, tiled=True)
    power = lax.all_gather(power, "section", axis=0, tiled=True)
    feeds_here = power.shape[1]
    power = power.reshape(LANES, OUTER, feeds_here).transpose(1, 2, 0)

    spectra = channelize(voltages, n_section)
    result = solve(spectra, power, n_section, n_chan)
    result = result.reshape(OUTER, 2, feeds_here, LANES)
    width = LANES // n_section
    result = lax.dynamic_slice_in_dim(result, lax.axis_index("section") * width, width, axis=3)
    result = result.transpose(1, 3, 0, 2).reshape(2, width * OUTER, feeds_here)
    result = lax.all_to_all(result, "chan", split_axis=1, concat_axis=2, tiled=True)
    result = result.astype(F32)
    length = jnp.sqrt(jnp.sum(result * result, axis=(0, 2)) + epsilon)
    return result / jnp.sqrt(length)[None, :, None]


def solution(mesh):
    in_specs = (
        P(None, "chan", "section"),
        P(("section", "chan"), None),
        P(("section", "chan"), None),
    )
    out_specs = P(None, ("section", "chan"), None)
    return jax.shard_map(local, mesh=mesh, in_specs=in_specs, out_specs=out_specs, check_vma=False)
```

```python
import functools
import math

import jax
import jax.numpy as jnp
import numpy as np
from jax import lax
from jax.experimental import pallas as pl
from jax.experimental.pallas import tpu as pltpu
from jax.sharding import PartitionSpec as P

CHANNELS = 4096
TAPS = 4
ITERS = 5
LANES = 128
OUTER = CHANNELS // LANES
TILE = 16
epsilon = 1e-06
F32 = jnp.float32
BF16 = jnp.bfloat16
VMEM_LIMIT = 60 * 1024 * 1024


def prototype():
    position = np.arange(TAPS * CHANNELS, dtype=np.float64)
    offset = (position - 0.5 * TAPS * CHANNELS + 0.5) / CHANNELS
    window = 0.5 - 0.5 * np.cos(2.0 * np.pi * (position + 0.5) / (TAPS * CHANNELS))
    taps = np.sin(np.pi * offset) / (np.pi * offset) * window
    return taps.astype(np.float32).reshape(TAPS, OUTER, LANES)


def table_seed():
    j = np.arange(LANES)
    inner = np.exp(-2j * np.pi * (np.outer(j, j) % LANES) / LANES) / math.sqrt(CHANNELS)
    twist = np.exp(-2j * np.pi * np.repeat(j[:, None], LANES, axis=1) / CHANNELS)
    parts = np.stack([inner.real, inner.imag, twist.real, twist.imag])
    return jnp.asarray(parts.astype(np.float32))


def times(z, w):
    zr, zi = z
    wr, wi = float(w.real), float(w.imag)
    if abs(wi) < 1e-12 and abs(wr - 1) < 1e-12:
        return zr, zi
    if abs(wr) < 1e-12 and abs(wi + 1) < 1e-12:
        return zi, -zr
    half = math.sqrt(0.5)
    if abs(wr - half) < 1e-12 and abs(wi + half) < 1e-12:
        return (zr + zi) * half, (zi - zr) * half
    if abs(wr + half) < 1e-12 and abs(wi + half) < 1e-12:
        return (zi - zr) * half, (zr + zi) * -half
    return zr * wr - zi * wi, zr * wi + zi * wr


def plus(a, b):
    return a[0] + b[0], a[1] + b[1]


def minus(a, b):
    return a[0] - b[0], a[1] - b[1]


def dft(values):
    n = len(values)
    if n == 1:
        return values
    even, odd = dft(values[0::2]), dft(values[1::2])
    odd = [times(z, np.exp(-2j * np.pi * k / n)) for k, z in enumerate(odd)]
    return [plus(a, b) for a, b in zip(even, odd)] + [minus(a, b) for a, b in zip(even, odd)]


QUICK = 8
SLOW = OUTER // QUICK


def channelize_kernel(sizes, *refs):
    frames, tiles, early, n_section, n_chan = sizes
    (x_ref, prev_ref, taps_ref, seed_ref, whole_ref, power_ref, out_ref, all_power,
     filtered, quick, ah, al, bh, bl, high, low, turning, history, send_sem, recv_sem, power_ss, power_rs, own_sem) = refs
    rows = frames * TILE
    margin = (TAPS - 1) * CHANNELS
    step = pl.program_id(0)
    last = pl.num_programs(0) - 1
    me = lax.axis_index("section")
    n_dev = n_section * n_chan
    place = me * n_chan + lax.axis_index("chan")

    def power_copy(d, receive=False):
        to = (place + d) % n_dev
        owner = (place - d + n_dev) % n_dev if receive else place
        return pltpu.make_async_remote_copy(
            src_ref=power_ref.at[to % n_chan], dst_ref=all_power.at[owner],
            send_sem=power_ss.at[d - 1], recv_sem=power_rs.at[d - 1],
            device_id={"section": to // n_chan, "chan": to % n_chan},
            device_id_type=pl.DeviceIdType.MESH,
        )

    own_power = pltpu.make_async_copy(
        power_ref.at[place % n_chan], all_power.at[place], own_sem
    )

    def history_copy(tile):
        start = whole_ref.shape[2] - margin
        src = whole_ref.at[:, pl.ds(tile * TILE, TILE), pl.ds(start, margin)]
        return pltpu.make_async_remote_copy(
            src_ref=src, dst_ref=history.at[tile], send_sem=send_sem.at[tile],
            recv_sem=recv_sem.at[tile], device_id={"section": (me + 1) % n_section},
            device_id_type=pl.DeviceIdType.MESH,
        )

    @pl.when(step == 0)
    def _():
        barrier = pltpu.get_barrier_semaphore()

        @pl.loop(1, n_dev)
        def _(d):
            to = (place + d) % n_dev
            pl.semaphore_signal(barrier, inc=1,
                                device_id={"section": to // n_chan, "chan": to % n_chan},
                                device_id_type=pl.DeviceIdType.MESH)

        pl.semaphore_wait(barrier, n_dev - 1)

        @pl.when(me < n_section - 1)
        def _():
            for tile in range(tiles):
                history_copy(tile).start()

        own_power.start()

        @pl.loop(1, n_dev)
        def _(d):
            power_copy(d).start()

        @pl.when(me == 0)
        def _():
            def clear(i, carry):
                at = pl.ds(pl.multiple_of(i * LANES, LANES), LANES)
                for tile in range(tiles):
                    for part in range(2):
                        history[tile, part, :, at] = jnp.zeros((TILE, LANES), BF16)
                return carry

            lax.fori_loop(0, margin // LANES, clear, 0)

        turning[...] = seed_ref[0:2]

        def build(k1, carry):
            for r in range(0, LANES, TILE):
                at = slice(r, r + TILE)
                below = slice(LANES + r, LANES + r + TILE)
                re, im = turning[0, at, :], turning[1, at, :]
                for rows_at, left, value in ((at, 0, re), (at, LANES, im),
                                             (below, 0, -im), (below, LANES, re)):
                    top = value.astype(BF16)
                    columns = slice(left, left + LANES)
                    high[k1, rows_at, columns] = top
                    low[k1, rows_at, columns] = (value - top.astype(F32)).astype(BF16)
                tr, ti = seed_ref[2, at, :], seed_ref[3, at, :]
                turning[0, at, :] = re * tr - im * ti
                turning[1, at, :] = re * ti + im * tr
            return carry

        lax.fori_loop(0, OUTER, build, 0)

    def run_filter(before):
        def filter_step(m, carry):
            column = m * LANES
            taps = [taps_ref[t, pl.ds(m, 1), :] for t in range(TAPS)]
            for part in range(2):
                window = []
                for frame in range(1 - TAPS, frames):
                    if frame < 0:
                        tile = before(frame, part, column)
                    else:
                        at = pl.multiple_of(frame * CHANNELS + column, LANES)
                        tile = x_ref[part, :, pl.ds(at, LANES)]
                    window.append(tile.astype(F32))
                for b in range(frames):
                    total = window[b] * taps[0]
                    for t in range(1, TAPS):
                        total = total + window[b + t] * taps[t]
                    filtered[m, part, b * TILE : (b + 1) * TILE, :] = total
            return carry

        lax.fori_loop(0, OUTER, filter_step, 0)

    @pl.when(step < early)
    def _():
        def before(frame, part, column):
            at = pl.multiple_of((4 + frame) * CHANNELS + column, LANES)
            return prev_ref[part, :, pl.ds(at, LANES)]

        run_filter(before)

    @pl.when(step >= early)
    def _():
        tile = step - early

        @pl.when(me > 0)
        def _():
            history_copy(tile).wait_recv()

        def before(frame, part, column):
            at = pl.multiple_of((TAPS - 1 + frame) * CHANNELS + column, LANES)
            return history[tile, part, :, pl.ds(at, LANES)]

        run_filter(before)

    def quick_step(r, carry):
        at = pl.ds(pl.multiple_of(r * 8, 8), 8)
        for m0 in range(SLOW):
            values = [
                tuple(filtered[m1 * SLOW + m0, part, at, :] for part in range(2))
                for m1 in range(QUICK)
            ]
            for k, z in enumerate(dft(values)):
                z = times(z, np.exp(-2j * np.pi * m0 * k / OUTER))
                for part in range(2):
                    quick[k, m0, part, at, :] = z[part]
        return carry

    lax.fori_loop(0, rows // 8, quick_step, 0)

    def slow_step(k, hi_ref, lo_ref):
        for r in range(0, rows, TILE):
            at = slice(r, r + TILE)
            values = [
                tuple(quick[k, m0, part, at, :] for part in range(2)) for m0 in range(SLOW)
            ]
            for i, z in enumerate(dft(values)):
                for part in range(2):
                    hi = z[part].astype(BF16)
                    lo = (z[part] - hi.astype(F32)).astype(BF16)
                    hi_ref[i, part, at, :] = hi
                    lo_ref[i, part, at, :] = lo

    def matmul_step(k, hi_ref, lo_ref):
        for i in range(SLOW):
            k1 = i * QUICK + k
            hi = jnp.concatenate([hi_ref[i, 0], hi_ref[i, 1]], axis=1)
            lo = jnp.concatenate([lo_ref[i, 0], lo_ref[i, 1]], axis=1)
            th, tl = high[k1], low[k1]
            dot = functools.partial(jnp.dot, preferred_element_type=F32)
            res = (dot(hi, th) + dot(lo, th)) + dot(hi, tl)
            for part in range(2):
                piece = res[:, part * LANES : (part + 1) * LANES].astype(BF16)
                out_ref[k1, part, 0] = piece.reshape(frames, TILE, LANES)

    slow_step(0, ah, al)

    def pair_step(i, carry):
        k = 2 * i
        slow_step(k + 1, bh, bl)
        matmul_step(k, ah, al)
        slow_step(jnp.minimum(k + 2, QUICK - 1), ah, al)
        matmul_step(k + 1, bh, bl)
        return carry

    lax.fori_loop(0, QUICK // 2, pair_step, 0)

    @pl.when((step == last) & (me < n_section - 1))
    def _():
        for tile in range(tiles):
            history_copy(tile).wait_send()

    @pl.when(step == last)
    def _():
        own_power.wait()

        @pl.loop(1, n_dev)
        def _(d):
            power_copy(d).wait_send()
            power_copy(d, receive=True).wait_recv()


def channelize(voltages, power, n_section, n_chan):
    n_dev = n_section * n_chan
    feeds_here = voltages.shape[1]
    blocks = voltages.shape[2] // CHANNELS
    frames = 8
    tiles, groups = feeds_here // TILE, blocks // frames
    early = tiles * (groups - 1)
    rows = frames * TILE
    per = frames // 4

    def place(i):
        late = i >= early
        tile = jnp.where(late, i - early, i // (groups - 1))
        return tile, jnp.where(late, 0, 1 + i % (groups - 1))

    def x_map(i):
        tile, group = place(i)
        return 0, tile, group

    def prev_map(i):
        tile, group = place(jnp.minimum(i, early - 1))
        return 0, tile, group * per - 1

    def out_map(i):
        tile, group = place(i)
        return 0, 0, tile, group, 0, 0

    table = pltpu.VMEM((OUTER, 2 * LANES, 2 * LANES), BF16)
    half = pltpu.VMEM((SLOW, 2, rows, LANES), BF16)
    return pl.pallas_call(
        functools.partial(channelize_kernel, (frames, tiles, early, n_section, n_chan)),
        grid=(tiles * groups,),
        in_specs=[
            pl.BlockSpec((2, TILE, frames * CHANNELS), x_map),
            pl.BlockSpec((2, TILE, 4 * CHANNELS), prev_map),
            pl.BlockSpec((TAPS, OUTER, LANES), lambda i: (0, 0, 0)),
            pl.BlockSpec((4, LANES, LANES), lambda i: (0, 0, 0)),
            pl.BlockSpec(memory_space=pl.ANY),
            pl.BlockSpec(memory_space=pl.ANY),
        ],
        out_specs=[
            pl.BlockSpec((OUTER, 2, 1, frames, TILE, LANES), out_map),
            pl.BlockSpec(memory_space=pl.ANY),
        ],
        out_shape=[
            jax.ShapeDtypeStruct((OUTER, 2, tiles, blocks, TILE, LANES), BF16),
            jax.ShapeDtypeStruct((n_dev,) + power.shape[1:], BF16),
        ],
        scratch_shapes=[
            pltpu.VMEM((OUTER, 2, rows + 8, LANES), F32),
            pltpu.VMEM((QUICK, SLOW, 2, rows + 8, LANES), F32),
            half, half, half, half, table, table,
            pltpu.VMEM((2, LANES, LANES), F32),
            pltpu.VMEM((tiles, 2, TILE, (TAPS - 1) * CHANNELS), BF16),
            pltpu.SemaphoreType.DMA((tiles,)),
            pltpu.SemaphoreType.DMA((tiles,)),
            pltpu.SemaphoreType.DMA((n_dev - 1,)),
            pltpu.SemaphoreType.DMA((n_dev - 1,)),
            pltpu.SemaphoreType.DMA,
        ],
        compiler_params=pltpu.CompilerParams(
            dimension_semantics=("arbitrary",), vmem_limit_bytes=VMEM_LIMIT,
            collective_id=0, has_side_effects=True,
        ),
    )(voltages, voltages, jnp.asarray(prototype()), table_seed(), voltages, power)


def fold_rows(parts):
    row = lax.broadcasted_iota(jnp.int32, (8, LANES), 0)
    half = []
    for i in range(4):
        a, b = parts[i], parts[i + 4]
        keep = jnp.where(row < 4, a, b)
        move = jnp.where(row < 4, b, a)
        half.append(keep + pltpu.roll(move, 4, 0))
    for shift in (2, 1):
        count = len(half) // 2
        bit = (row & shift) == 0
        half = [
            jnp.where(
                bit,
                half[i] + pltpu.roll(half[i], 8 - shift, 0),
                half[i + count] + pltpu.roll(half[i + count], shift, 0),
            )
            for i in range(count)
        ]
    return half[0]


def solve_kernel(sizes, *refs):
    n_section, n_chan, feeds, blocks, chunks, kc = sizes
    (spectra_hbm, power_ref, out_ref,
     spectra, diagonal, local_p, half_in, half_sum, half_out, piece_in, full_p, scaled,
     norm, local_q, q_in, y_ref,
     load_sem, half_ss, half_rs, piece_ss, piece_rs, gather_ss, gather_rs,
     share_ss, share_rs, norm_ss, norm_rs, q_ss, q_rs, y_ss, y_rs,
     turned, final_ss, final_rs, own_sem) = refs
    tiles = feeds // TILE
    n_z = n_chan // 2
    me_s = lax.axis_index("section")
    me_c = lax.axis_index("chan")
    n_dev = n_section * n_chan
    me = me_s * n_chan + me_c
    share = LANES // n_dev
    core, z = me_c % 2, me_c // 2
    half_k = kc // 2
    half_rows = half_k * 2 * blocks
    piece_rows = half_rows // n_z
    k_piece = kc // n_section

    def remote(src, dst, ss, rs, **where):
        return pltpu.make_async_remote_copy(
            src_ref=src, dst_ref=dst, send_sem=ss, recv_sem=rs,
            device_id=where, device_id_type=pl.DeviceIdType.MESH,
        )

    def load(c):
        at = pl.ds(c * kc, kc)
        return pltpu.make_async_copy(spectra_hbm.at[at], spectra.at[at], load_sem.at[c])

    def half_copy(c):
        return remote(local_p.at[c, 1 - core], half_in.at[c], half_ss.at[c], half_rs.at[c],
                      chan=z * 2 + (1 - core))

    def norm_copies(c):
        return [
            remote(norm.at[c, 0], norm.at[c, d], norm_ss.at[c, d - 1], norm_rs.at[c, d - 1],
                   chan=(me_c + d) % n_chan)
            for d in range(1, n_chan)
        ]

    def piece_copies(c):
        copies = []
        for d in range(1, n_z):
            to = (z + d) % n_z
            rows = pl.ds(pl.multiple_of(to * piece_rows, piece_rows), piece_rows)
            copies.append(remote(half_out.at[c, rows], piece_in.at[c, d - 1],
                                 piece_ss.at[c, d - 1], piece_rs.at[c, d - 1],
                                 chan=to * 2 + core))
        return copies

    def gather_copies(c, receive=False):
        copies = []
        for d in range(1, n_z):
            to = (z + d) % n_z
            owner = (z - d + n_z) % n_z if receive else z
            rows = pl.ds(pl.multiple_of(owner * piece_rows, piece_rows), piece_rows)
            view = full_p.at[c, core, rows]
            copies.append(remote(view, view, gather_ss.at[c, d - 1], gather_rs.at[c, d - 1],
                                 chan=to * 2 + core))
        return copies

    def share_copy(c, receive=False):
        view = full_p.at[c, 1 - core if receive else core]
        return remote(view, view, share_ss.at[c], share_rs.at[c], chan=z * 2 + (1 - core))

    def q_copies(c):
        copies = []
        for d in range(1, n_section):
            to = (me_s + d) % n_section
            copies.append(remote(local_q.at[c, pl.ds(to * k_piece, k_piece)], q_in.at[c, d - 1],
                                 q_ss.at[c, d - 1], q_rs.at[c, d - 1], section=to))
        return copies

    def y_copies(c, receive=False):
        copies = []
        for d in range(1, n_section):
            to = (me_s + d) % n_section
            owner = (me_s - d + n_section) % n_section if receive else me_s
            view = y_ref.at[c, pl.ds(owner * k_piece, k_piece)]
            copies.append(remote(view, view, y_ss.at[c, d - 1], y_rs.at[c, d - 1], section=to))
        return copies

    def pair(k1, tile, b):
        return spectra[k1, 0, tile, b].astype(F32), spectra[k1, 1, tile, b].astype(F32)

    def store_rows(c, k, g, rows_r, rows_i):
        at = (k % half_k) * (2 * blocks) + g * 8
        h = k // half_k
        local_p[c, h, pl.ds(pl.multiple_of(at, 8), 8), :] = fold_rows(rows_r)
        at = at + blocks
        local_p[c, h, pl.ds(pl.multiple_of(at, 8), 8), :] = fold_rows(rows_i)

    def project(it, c):
        @pl.when(it == 0)
        def _():
            load(c).wait()

            def one(k, carry):
                k1 = c * kc + k
                power = [power_ref[k1, t * TILE : (t + 1) * TILE, :].astype(F32)
                         for t in range(tiles)]
                weight = [jnp.where(p > 0, 1.0, 0.0) for p in power]

                def group(g, totals):
                    totals = list(totals)
                    rows_r, rows_i = [], []
                    for s in range(8):
                        b = g * 8 + s
                        ar = ai = jnp.zeros((TILE, LANES), F32)
                        for t in range(tiles):
                            re, im = pair(k1, t, b)
                            ar = ar + re * weight[t]
                            ai = ai - im * weight[t]
                            totals[t] = totals[t] + (re * re + im * im)
                        rows_r.append(ar[:8] + ar[8:])
                        rows_i.append(ai[:8] + ai[8:])
                    store_rows(c, k, g, rows_r, rows_i)
                    return tuple(totals)

                zero = jnp.zeros((TILE, LANES), F32)
                totals = lax.fori_loop(0, blocks // 8, group, (zero,) * tiles)
                for t in range(tiles):
                    at = slice(t * TILE, (t + 1) * TILE)
                    diagonal[k1, at, :] = blocks * power[t] - totals[t]
                return carry

            lax.fori_loop(0, kc, one, 0)

        @pl.when(it > 0)
        def _():
            for copy in y_copies(c):
                copy.wait_send()
            for copy in y_copies(c, receive=True):
                copy.wait_recv()

            def one(k, carry):
                k1 = c * kc + k
                yr, yi = ([y_ref[c, k, part, t * TILE : (t + 1) * TILE, :].astype(F32)
                           for t in range(tiles)] for part in range(2))
                square = sum(a * a for a in yr + yi)
                norm[c, 0, pl.ds(k, 1), :] = jnp.sum(square, axis=0, keepdims=True)

                less = [b - a for a, b in zip(yr, yi)]
                more = [b + a for a, b in zip(yr, yi)]

                def group(g, carry):
                    rows_r, rows_i = [], []
                    for s in range(8):
                        b = g * 8 + s
                        one = two = three = None
                        for t in range(tiles):
                            re, im = pair(k1, t, b)
                            x, y, z = (re - im) * yr[t], re * less[t], im * more[t]
                            one, two, three = (x, y, z) if t == 0 else (one + x, two + y, three + z)
                        one = one[:8] + one[8:]
                        rows_r.append(one + (three[:8] + three[8:]))
                        rows_i.append(one + (two[:8] + two[8:]))
                    store_rows(c, k, g, rows_r, rows_i)
                    return carry

                lax.fori_loop(0, blocks // 8, group, 0)
                return carry

            lax.fori_loop(0, kc, one, 0)

        half_copy(c).start()
        for copy in norm_copies(c):
            copy.start()

    def add_half(it, c):
        half_copy(c).wait()
        total = local_p[c, core] + half_in[c]
        half_sum[c] = total
        half_out[c] = total.astype(BF16)
        for copy in piece_copies(c):
            copy.start()

    def add_pieces(it, c):
        for copy in piece_copies(c):
            copy.wait()
        rows = pl.ds(pl.multiple_of(z * piece_rows, piece_rows), piece_rows)
        total = half_sum[c, rows, :]
        for d in range(1, n_z):
            total = total + piece_in[c, d - 1].astype(F32)
        full_p[c, core, rows, :] = total
        for copy in gather_copies(c):
            copy.start()

    def share_half(it, c):
        for copy in gather_copies(c):
            copy.wait_send()
        for copy in gather_copies(c, receive=True):
            copy.wait_recv()
        share_copy(c).start()

    def expand(it, c):
        share_copy(c).wait_send()
        share_copy(c, receive=True).wait_recv()
        for copy in norm_copies(c):
            copy.wait()
        length = norm[c, 0]
        for d in range(1, n_chan):
            length = length + norm[c, d]
        inverse = jnp.where(it == 0, 1.0, 1.0 / jnp.sqrt(length + epsilon))
        scaled[pl.ds(3 * blocks, kc), :] = inverse

        def one(k, carry):
            k1 = c * kc + k
            inv = scaled[pl.ds(3 * blocks + k, 1), :]
            at = pl.multiple_of((k % half_k) * (2 * blocks), 2 * blocks)
            real = full_p[c, k // half_k, pl.ds(at, blocks), :] * inv
            at = pl.multiple_of(at + blocks, blocks)
            imag = full_p[c, k // half_k, pl.ds(at, blocks), :] * inv
            scaled[0:blocks, :] = real
            scaled[blocks : 2 * blocks, :] = imag - real
            scaled[2 * blocks : 3 * blocks, :] = imag + real

            def group(g, totals):
                totals = list(totals)
                for s in range(8):
                    b = g * 8 + s
                    pr, less, more = (scaled[pl.ds(i * blocks + b, 1), :] for i in range(3))
                    for t in range(tiles):
                        re, im = pair(k1, t, b)
                        totals[3 * t] = totals[3 * t] + (re + im) * pr
                        totals[3 * t + 1] = totals[3 * t + 1] + re * less
                        totals[3 * t + 2] = totals[3 * t + 2] + im * more
                return tuple(totals)

            zero = jnp.zeros((TILE, LANES), F32)
            totals = lax.fori_loop(0, blocks // 8, group, (zero,) * (3 * tiles))
            for t in range(tiles):
                at = slice(t * TILE, (t + 1) * TILE)
                usable = power_ref[k1, at, :].astype(F32) > 0
                shift = diagonal[k1, at, :] * inv
                sums = totals[3 * t] - totals[3 * t + 2], totals[3 * t] + totals[3 * t + 1]
                for part in range(2):
                    now = y_ref[c, k, part, at, :].astype(F32)
                    value = jnp.where(usable, sums[part] + shift * now, 0.0)
                    local_q[c, k, part, at, :] = value.astype(BF16)
            return carry

        lax.fori_loop(0, kc, one, 0)
        for copy in q_copies(c):
            copy.start()

    def final_copy(c, d):
        to = (me + d) % n_dev
        return remote(turned.at[c, to], out_ref.at[c, me], final_ss.at[c], final_rs.at[c],
                      section=to // n_chan, chan=to % n_chan)

    def own_copy(c):
        return pltpu.make_async_copy(turned.at[c, me], out_ref.at[c, me], own_sem.at[c])

    def final_wait(c):
        others = turned.at[c, pl.ds(0, n_dev - 1)]
        pltpu.make_async_copy(others, others, final_ss.at[c]).wait()
        others = out_ref.at[c, pl.ds(0, n_dev - 1)]
        pltpu.make_async_copy(others, others, final_rs.at[c]).wait()
        own_copy(c).wait()

    def section_sum(c, k, part):
        total = local_q[c, me_s * k_piece + k, part].astype(F32)
        for d in range(1, n_section):
            total = total + q_in[c, d - 1, k, part].astype(F32)
        return total

    def add_sections(it, c):
        for copy in q_copies(c):
            copy.wait()

        @pl.when(it < ITERS - 1)
        def _():
            for k in range(k_piece):
                for part in range(2):
                    y_ref[c, me_s * k_piece + k, part] = section_sum(c, k, part).astype(BF16)
            for copy in y_copies(c):
                copy.start()

        @pl.when(it == ITERS - 1)
        def _():
            for k in range(k_piece):
                parts = [section_sum(c, k, part) for part in range(2)]
                total = jnp.concatenate(parts, axis=0).T
                for to in range(n_dev):
                    turned[c, to, k] = total[to * share : (to + 1) * share]
            own_copy(c).start()

            @pl.loop(1, n_dev)
            def _(d):
                final_copy(c, d).start()

    barrier = pltpu.get_barrier_semaphore()

    @pl.loop(1, n_dev)
    def _(d):
        to = (me + d) % n_dev
        pl.semaphore_signal(barrier, inc=1,
                            device_id={"section": to // n_chan, "chan": to % n_chan},
                            device_id_type=pl.DeviceIdType.MESH)

    @pl.loop(0, chunks)
    def _(c):
        load(c).start()

    @pl.loop(0, chunks)
    def _(c):
        for k in range(kc):
            power = power_ref[c * kc + k].astype(F32)
            y_ref[c, k, 0] = jnp.where(power > 0, 1.0, 0.0).astype(BF16)
            y_ref[c, k, 1] = jnp.zeros((feeds, LANES), BF16)
        norm[c, 0] = jnp.zeros((kc, LANES), F32)

    pl.semaphore_wait(barrier, n_dev - 1)

    stages = [(7, add_sections), (3, add_pieces), (5, expand), (4, share_half), (1, add_half),
              (0, project)]
    span = 7
    period = max(chunks, span + 1)

    @pl.loop(0, ITERS * period + span)
    def _(slot):
        for lag, stage in stages:
            turn = slot - lag + period
            it, c = turn // period - 1, turn % period

            @pl.when((it >= 0) & (it < ITERS) & (c < chunks))
            def _():
                stage(it, c)

    @pl.loop(0, chunks)
    def _(c):
        final_wait(c)


def solve(spectra, power, n_section, n_chan):
    feeds, blocks = spectra.shape[2] * TILE, spectra.shape[3]
    kc = n_section
    chunks = OUTER // kc
    n_z = n_chan // 2
    half_rows = kc * blocks
    piece_rows = half_rows // n_z
    k_piece = kc // n_section
    n_dev = n_section * n_chan
    dma = pltpu.SemaphoreType.DMA
    per = lambda n: dma((chunks, n))
    scratch = [
        pltpu.VMEM(spectra.shape, BF16),
        pltpu.VMEM((OUTER, feeds, LANES), F32),
        pltpu.VMEM((chunks, 2, half_rows, LANES), F32),
        pltpu.VMEM((chunks, half_rows, LANES), F32),
        pltpu.VMEM((chunks, half_rows, LANES), F32),
        pltpu.VMEM((chunks, half_rows, LANES), BF16),
        pltpu.VMEM((chunks, n_z - 1, piece_rows, LANES), BF16),
        pltpu.VMEM((chunks, 2, half_rows, LANES), F32),
        pltpu.VMEM((3 * blocks + 8, LANES), F32),
        pltpu.VMEM((chunks, n_chan, kc, LANES), F32),
        pltpu.VMEM((chunks, kc, 2, feeds, LANES), BF16),
        pltpu.VMEM((chunks, n_section - 1, k_piece, 2, feeds, LANES), BF16),
        pltpu.VMEM((chunks, kc, 2, feeds, LANES), BF16),
        dma((chunks,)),
        dma((chunks,)), dma((chunks,)),
        per(n_z - 1), per(n_z - 1), per(n_z - 1), per(n_z - 1),
        dma((chunks,)), dma((chunks,)),
        per(n_chan - 1), per(n_chan - 1),
        per(n_section - 1), per(n_section - 1), per(n_section - 1), per(n_section - 1),
        pltpu.VMEM((chunks, n_dev, k_piece, LANES // n_dev, 2 * feeds), F32),
        dma((chunks,)), dma((chunks,)), dma((chunks,)),
    ]
    vmem = pl.BlockSpec(memory_space=pltpu.VMEM)
    return pl.pallas_call(
        functools.partial(solve_kernel, (n_section, n_chan, feeds, blocks, chunks, kc)),
        in_specs=[pl.BlockSpec(memory_space=pl.ANY), vmem],
        out_specs=pl.BlockSpec(memory_space=pl.ANY),
        out_shape=jax.ShapeDtypeStruct(
            (chunks, n_dev, k_piece, LANES // n_dev, 2 * feeds), F32
        ),
        scratch_shapes=scratch,
        compiler_params=pltpu.CompilerParams(
            collective_id=1, has_side_effects=True, vmem_limit_bytes=VMEM_LIMIT
        ),
    )(spectra, power)


def local(voltages, usable, auto_power):
    n_section, n_chan = lax.axis_size("section"), lax.axis_size("chan")
    power = (usable.astype(F32) * auto_power).astype(BF16)
    here = power.shape[0]
    feeds_here = power.shape[1] // n_chan
    pack = LANES // feeds_here
    power = power.reshape(pack, here // pack, n_chan, feeds_here).transpose(2, 1, 0, 3)
    power = power.reshape(n_chan, here // pack, LANES)

    spectra, power = channelize(voltages, power, n_section, n_chan)
    power = power.reshape(-1, here // pack, pack, feeds_here).transpose(0, 2, 1, 3)
    power = power.reshape(LANES, OUTER, feeds_here).transpose(1, 2, 0)
    result = solve(spectra, power, n_section, n_chan)
    chunks, k_piece = result.shape[0], result.shape[2]
    result = result.reshape(chunks, n_section, n_chan, k_piece, -1, 2, feeds_here)
    result = result.transpose(5, 4, 0, 1, 3, 2, 6).reshape(2, here, n_chan * feeds_here)
    length = jnp.sqrt(jnp.sum(result * result, axis=(0, 2)) + epsilon)
    return result / jnp.sqrt(length)[None, :, None]


def solution(mesh):
    in_specs = (
        P(None, "chan", "section"),
        P(("section", "chan"), None),
        P(("section", "chan"), None),
    )
    out_specs = P(None, ("section", "chan"), None)
    return jax.shard_map(local, mesh=mesh, in_specs=in_specs, out_specs=out_specs, check_vma=False)
```

```python
import functools
import math

import jax
import jax.numpy as jnp
import numpy as np
from jax import lax
from jax.experimental import pallas as pl
from jax.experimental.pallas import tpu as pltpu
from jax.sharding import PartitionSpec as P

CHANNELS = 4096
TAPS = 4
ITERS = 5
LANES = 128
OUTER = CHANNELS // LANES
TILE = 16
epsilon = 1e-06
F32 = jnp.float32
BF16 = jnp.bfloat16
VMEM_LIMIT = 60 * 1024 * 1024


def prototype():
    position = np.arange(TAPS * CHANNELS, dtype=np.float64)
    offset = (position - 0.5 * TAPS * CHANNELS + 0.5) / CHANNELS
    window = 0.5 - 0.5 * np.cos(2.0 * np.pi * (position + 0.5) / (TAPS * CHANNELS))
    taps = np.sin(np.pi * offset) / (np.pi * offset) * window
    return taps.astype(np.float32).reshape(TAPS, OUTER, LANES)


def table_seed():
    j = np.arange(LANES)
    inner = np.exp(-2j * np.pi * (np.outer(j, j) % LANES) / LANES) / math.sqrt(CHANNELS)
    twist = np.exp(-2j * np.pi * np.repeat(j[:, None], LANES, axis=1) / CHANNELS)
    parts = np.stack([inner.real, inner.imag, twist.real, twist.imag])
    return jnp.asarray(parts.astype(np.float32))


def times(z, w):
    zr, zi = z
    wr, wi = float(w.real), float(w.imag)
    if abs(wi) < 1e-12 and abs(wr - 1) < 1e-12:
        return zr, zi
    if abs(wr) < 1e-12 and abs(wi + 1) < 1e-12:
        return zi, -zr
    half = math.sqrt(0.5)
    if abs(wr - half) < 1e-12 and abs(wi + half) < 1e-12:
        return (zr + zi) * half, (zi - zr) * half
    if abs(wr + half) < 1e-12 and abs(wi + half) < 1e-12:
        return (zi - zr) * half, (zr + zi) * -half
    return zr * wr - zi * wi, zr * wi + zi * wr


def plus(a, b):
    return a[0] + b[0], a[1] + b[1]


def minus(a, b):
    return a[0] - b[0], a[1] - b[1]


def dft(values):
    n = len(values)
    if n == 1:
        return values
    even, odd = dft(values[0::2]), dft(values[1::2])
    sums, differences = [], []
    for k, (a, z) in enumerate(zip(even, odd)):
        if 4 * k == n:
            sums.append((a[0] + z[1], a[1] - z[0]))
            differences.append((a[0] - z[1], a[1] + z[0]))
        else:
            z = times(z, np.exp(-2j * np.pi * k / n))
            sums.append(plus(a, z))
            differences.append(minus(a, z))
    return sums + differences


QUICK = 8
SLOW = OUTER // QUICK


def channelize_kernel(sizes, *refs):
    frames, tiles, early, n_section, n_chan = sizes
    (x_ref, prev_ref, taps_ref, seed_ref, whole_ref, power_ref, out_ref, all_power,
     filtered, quick, ah, al, bh, bl, high, low, turning, history, send_sem, recv_sem, power_ss, power_rs, own_sem) = refs
    rows = frames * TILE
    margin = (TAPS - 1) * CHANNELS
    step = pl.program_id(0)
    last = pl.num_programs(0) - 1
    me = lax.axis_index("section")
    n_dev = n_section * n_chan
    place = me * n_chan + lax.axis_index("chan")

    def power_copy(d, receive=False):
        to = (place + d) % n_dev
        owner = (place - d + n_dev) % n_dev if receive else place
        return pltpu.make_async_remote_copy(
            src_ref=power_ref.at[to % n_chan], dst_ref=all_power.at[owner],
            send_sem=power_ss.at[d - 1], recv_sem=power_rs.at[d - 1],
            device_id={"section": to // n_chan, "chan": to % n_chan},
            device_id_type=pl.DeviceIdType.MESH,
        )

    own_power = pltpu.make_async_copy(
        power_ref.at[place % n_chan], all_power.at[place], own_sem
    )

    def history_copy(tile):
        start = whole_ref.shape[2] - margin
        src = whole_ref.at[:, pl.ds(tile * TILE, TILE), pl.ds(start, margin)]
        return pltpu.make_async_remote_copy(
            src_ref=src, dst_ref=history.at[tile], send_sem=send_sem.at[tile],
            recv_sem=recv_sem.at[tile], device_id={"section": (me + 1) % n_section},
            device_id_type=pl.DeviceIdType.MESH,
        )

    @pl.when(step == 0)
    def _():
        barrier = pltpu.get_barrier_semaphore()

        @pl.loop(1, n_dev)
        def _(d):
            to = (place + d) % n_dev
            pl.semaphore_signal(barrier, inc=1,
                                device_id={"section": to // n_chan, "chan": to % n_chan},
                                device_id_type=pl.DeviceIdType.MESH)

        pl.semaphore_wait(barrier, n_dev - 1)

        @pl.when(me < n_section - 1)
        def _():
            for tile in range(tiles):
                history_copy(tile).start()

        own_power.start()

        @pl.loop(1, n_dev)
        def _(d):
            power_copy(d).start()

        @pl.when(me == 0)
        def _():
            def clear(i, carry):
                at = pl.ds(pl.multiple_of(i * LANES, LANES), LANES)
                for tile in range(tiles):
                    for part in range(2):
                        history[tile, part, :, at] = jnp.zeros((TILE, LANES), BF16)
                return carry

            lax.fori_loop(0, margin // LANES, clear, 0)

        turning[...] = seed_ref[0:2]

        def build(k1, carry):
            for r in range(0, LANES, TILE):
                at = slice(r, r + TILE)
                below = slice(LANES + r, LANES + r + TILE)
                re, im = turning[0, at, :], turning[1, at, :]
                for rows_at, left, value in ((at, 0, re), (at, LANES, im),
                                             (below, 0, -im), (below, LANES, re)):
                    top = value.astype(BF16)
                    columns = slice(left, left + LANES)
                    high[k1, rows_at, columns] = top
                    low[k1, rows_at, columns] = (value - top.astype(F32)).astype(BF16)
                tr, ti = seed_ref[2, at, :], seed_ref[3, at, :]
                turning[0, at, :] = re * tr - im * ti
                turning[1, at, :] = re * ti + im * tr
            return carry

        lax.fori_loop(0, OUTER, build, 0)

    def run_filter(before):
        def filter_step(m, carry):
            column = m * LANES
            taps = [taps_ref[t, pl.ds(m, 1), :] for t in range(TAPS)]
            for part in range(2):
                window = []
                for frame in range(1 - TAPS, frames):
                    if frame < 0:
                        tile = before(frame, part, column)
                    else:
                        at = pl.multiple_of(frame * CHANNELS + column, LANES)
                        tile = x_ref[part, :, pl.ds(at, LANES)]
                    window.append(tile.astype(F32))
                for b in range(frames):
                    total = window[b] * taps[0]
                    for t in range(1, TAPS):
                        total = total + window[b + t] * taps[t]
                    filtered[m, part, b * TILE : (b + 1) * TILE, :] = total
            return carry

        lax.fori_loop(0, OUTER, filter_step, 0)

    @pl.when(step < early)
    def _():
        def before(frame, part, column):
            at = pl.multiple_of((4 + frame) * CHANNELS + column, LANES)
            return prev_ref[part, :, pl.ds(at, LANES)]

        run_filter(before)

    @pl.when(step >= early)
    def _():
        tile = step - early

        @pl.when(me > 0)
        def _():
            history_copy(tile).wait_recv()

        def before(frame, part, column):
            at = pl.multiple_of((TAPS - 1 + frame) * CHANNELS + column, LANES)
            return history[tile, part, :, pl.ds(at, LANES)]

        run_filter(before)

    def quick_step(r, carry):
        at = pl.ds(pl.multiple_of(r * 8, 8), 8)
        for m0 in range(SLOW):
            values = [
                tuple(filtered[m1 * SLOW + m0, part, at, :] for part in range(2))
                for m1 in range(QUICK)
            ]
            for k, z in enumerate(dft(values)):
                z = times(z, np.exp(-2j * np.pi * m0 * k / OUTER))
                for part in range(2):
                    quick[k, m0, part, at, :] = z[part]
        return carry

    lax.fori_loop(0, rows // 8, quick_step, 0)

    def slow_step(k, hi_ref, lo_ref):
        for r in range(0, rows, TILE):
            at = slice(r, r + TILE)
            values = [
                tuple(quick[k, m0, part, at, :] for part in range(2)) for m0 in range(SLOW)
            ]
            for i, z in enumerate(dft(values)):
                for part in range(2):
                    hi = z[part].astype(BF16)
                    lo = (z[part] - hi.astype(F32)).astype(BF16)
                    hi_ref[i, part, at, :] = hi
                    lo_ref[i, part, at, :] = lo

    def matmul_step(k, hi_ref, lo_ref):
        for i in range(SLOW):
            k1 = i * QUICK + k
            hi = jnp.concatenate([hi_ref[i, 0], hi_ref[i, 1]], axis=1)
            lo = jnp.concatenate([lo_ref[i, 0], lo_ref[i, 1]], axis=1)
            th, tl = high[k1], low[k1]
            dot = functools.partial(jnp.dot, preferred_element_type=F32)
            both = dot(jnp.concatenate([hi, lo], axis=0), th)
            res = (both[:rows] + both[rows:]) + dot(hi, tl)
            for part in range(2):
                piece = res[:, part * LANES : (part + 1) * LANES].astype(BF16)
                out_ref[k1, part, 0] = piece.reshape(frames, TILE, LANES)

    slow_step(0, ah, al)

    def pair_step(i, carry):
        k = 2 * i
        slow_step(k + 1, bh, bl)
        matmul_step(k, ah, al)
        slow_step(jnp.minimum(k + 2, QUICK - 1), ah, al)
        matmul_step(k + 1, bh, bl)
        return carry

    lax.fori_loop(0, QUICK // 2, pair_step, 0)

    @pl.when((step == last) & (me < n_section - 1))
    def _():
        for tile in range(tiles):
            history_copy(tile).wait_send()

    @pl.when(step == last)
    def _():
        own_power.wait()

        @pl.loop(1, n_dev)
        def _(d):
            power_copy(d).wait_send()
            power_copy(d, receive=True).wait_recv()


def channelize(voltages, power, n_section, n_chan):
    n_dev = n_section * n_chan
    feeds_here = voltages.shape[1]
    blocks = voltages.shape[2] // CHANNELS
    frames = 8
    tiles, groups = feeds_here // TILE, blocks // frames
    early = tiles * (groups - 1)
    rows = frames * TILE
    per = frames // 4

    def place(i):
        late = i >= early
        tile = jnp.where(late, i - early, i // (groups - 1))
        return tile, jnp.where(late, 0, 1 + i % (groups - 1))

    def x_map(i):
        tile, group = place(i)
        return 0, tile, group

    def prev_map(i):
        tile, group = place(jnp.minimum(i, early - 1))
        return 0, tile, group * per - 1

    def out_map(i):
        tile, group = place(i)
        return 0, 0, tile, group, 0, 0

    table = pltpu.VMEM((OUTER, 2 * LANES, 2 * LANES), BF16)
    half = pltpu.VMEM((SLOW, 2, rows, LANES), BF16)
    return pl.pallas_call(
        functools.partial(channelize_kernel, (frames, tiles, early, n_section, n_chan)),
        grid=(tiles * groups,),
        in_specs=[
            pl.BlockSpec((2, TILE, frames * CHANNELS), x_map),
            pl.BlockSpec((2, TILE, 4 * CHANNELS), prev_map),
            pl.BlockSpec((TAPS, OUTER, LANES), lambda i: (0, 0, 0)),
            pl.BlockSpec((4, LANES, LANES), lambda i: (0, 0, 0)),
            pl.BlockSpec(memory_space=pl.ANY),
            pl.BlockSpec(memory_space=pl.ANY),
        ],
        out_specs=[
            pl.BlockSpec((OUTER, 2, 1, frames, TILE, LANES), out_map),
            pl.BlockSpec(memory_space=pl.ANY),
        ],
        out_shape=[
            jax.ShapeDtypeStruct((OUTER, 2, tiles, blocks, TILE, LANES), BF16),
            jax.ShapeDtypeStruct((n_dev,) + power.shape[1:], BF16),
        ],
        scratch_shapes=[
            pltpu.VMEM((OUTER, 2, rows + 8, LANES), F32),
            pltpu.VMEM((QUICK, SLOW, 2, rows + 8, LANES), F32),
            half, half, half, half, table, table,
            pltpu.VMEM((2, LANES, LANES), F32),
            pltpu.VMEM((tiles, 2, TILE, (TAPS - 1) * CHANNELS), BF16),
            pltpu.SemaphoreType.DMA((tiles,)),
            pltpu.SemaphoreType.DMA((tiles,)),
            pltpu.SemaphoreType.DMA((n_dev - 1,)),
            pltpu.SemaphoreType.DMA((n_dev - 1,)),
            pltpu.SemaphoreType.DMA,
        ],
        compiler_params=pltpu.CompilerParams(
            dimension_semantics=("arbitrary",), vmem_limit_bytes=VMEM_LIMIT,
            collective_id=0, has_side_effects=True,
        ),
    )(voltages, voltages, jnp.asarray(prototype()), table_seed(), voltages, power)


def fold_rows(parts):
    row = lax.broadcasted_iota(jnp.int32, (8, LANES), 0)
    half = []
    for i in range(4):
        a, b = parts[i], parts[i + 4]
        keep = jnp.where(row < 4, a, b)
        move = jnp.where(row < 4, b, a)
        half.append(keep + pltpu.roll(move, 4, 0))
    for shift in (2, 1):
        count = len(half) // 2
        bit = (row & shift) == 0
        half = [
            jnp.where(
                bit,
                half[i] + pltpu.roll(half[i], 8 - shift, 0),
                half[i + count] + pltpu.roll(half[i + count], shift, 0),
            )
            for i in range(count)
        ]
    return half[0]


def solve_kernel(sizes, *refs):
    n_section, n_chan, feeds, blocks, chunks, kc = sizes
    (spectra_hbm, power_ref, out_ref,
     spectra, diagonal, local_p, half_in, half_sum, half_out, piece_in, full_p, scaled,
     norm, local_q, q_in, y_ref,
     load_sem, half_ss, half_rs, piece_ss, piece_rs, gather_ss, gather_rs,
     share_ss, share_rs, norm_ss, norm_rs, q_ss, q_rs, y_ss, y_rs,
     turned, final_ss, final_rs, own_sem) = refs
    tiles = feeds // TILE
    n_z = n_chan // 2
    me_s = lax.axis_index("section")
    me_c = lax.axis_index("chan")
    n_dev = n_section * n_chan
    me = me_s * n_chan + me_c
    share = LANES // n_dev
    core, z = me_c % 2, me_c // 2
    half_k = kc // 2
    half_rows = half_k * 2 * blocks
    piece_rows = half_rows // n_z
    k_piece = kc // n_section

    def remote(src, dst, ss, rs, **where):
        return pltpu.make_async_remote_copy(
            src_ref=src, dst_ref=dst, send_sem=ss, recv_sem=rs,
            device_id=where, device_id_type=pl.DeviceIdType.MESH,
        )

    def load(c):
        at = pl.ds(c * kc, kc)
        return pltpu.make_async_copy(spectra_hbm.at[at], spectra.at[at], load_sem.at[c])

    def half_copy(c):
        return remote(local_p.at[c, 1 - core], half_in.at[c], half_ss.at[c], half_rs.at[c],
                      chan=z * 2 + (1 - core))

    def norm_copies(c):
        return [
            remote(norm.at[c, 0], norm.at[c, d], norm_ss.at[c, d - 1], norm_rs.at[c, d - 1],
                   chan=(me_c + d) % n_chan)
            for d in range(1, n_chan)
        ]

    def piece_copies(c):
        copies = []
        for d in range(1, n_z):
            to = (z + d) % n_z
            rows = pl.ds(pl.multiple_of(to * piece_rows, piece_rows), piece_rows)
            copies.append(remote(half_out.at[c, rows], piece_in.at[c, d - 1],
                                 piece_ss.at[c, d - 1], piece_rs.at[c, d - 1],
                                 chan=to * 2 + core))
        return copies

    def gather_copies(c, receive=False):
        copies = []
        for d in range(1, n_z):
            to = (z + d) % n_z
            owner = (z - d + n_z) % n_z if receive else z
            rows = pl.ds(pl.multiple_of(owner * piece_rows, piece_rows), piece_rows)
            view = full_p.at[c, core, rows]
            copies.append(remote(view, view, gather_ss.at[c, d - 1], gather_rs.at[c, d - 1],
                                 chan=to * 2 + core))
        return copies

    def share_copy(c, receive=False):
        view = full_p.at[c, 1 - core if receive else core]
        return remote(view, view, share_ss.at[c], share_rs.at[c], chan=z * 2 + (1 - core))

    def q_copies(c):
        copies = []
        for d in range(1, n_section):
            to = (me_s + d) % n_section
            copies.append(remote(local_q.at[c, pl.ds(to * k_piece, k_piece)], q_in.at[c, d - 1],
                                 q_ss.at[c, d - 1], q_rs.at[c, d - 1], section=to))
        return copies

    def y_copies(c, receive=False):
        copies = []
        for d in range(1, n_section):
            to = (me_s + d) % n_section
            owner = (me_s - d + n_section) % n_section if receive else me_s
            view = y_ref.at[c, pl.ds(owner * k_piece, k_piece)]
            copies.append(remote(view, view, y_ss.at[c, d - 1], y_rs.at[c, d - 1], section=to))
        return copies

    def pair(k1, tile, b):
        return spectra[k1, 0, tile, b].astype(F32), spectra[k1, 1, tile, b].astype(F32)

    def store_rows(c, k, g, rows_r, rows_i):
        at = (k % half_k) * (2 * blocks) + g * 8
        h = k // half_k
        local_p[c, h, pl.ds(pl.multiple_of(at, 8), 8), :] = fold_rows(rows_r)
        at = at + blocks
        local_p[c, h, pl.ds(pl.multiple_of(at, 8), 8), :] = fold_rows(rows_i)

    def project(it, c):
        @pl.when(it == 0)
        def _():
            load(c).wait()

            def one(k, carry):
                k1 = c * kc + k
                power = [power_ref[k1, t * TILE : (t + 1) * TILE, :].astype(F32)
                         for t in range(tiles)]
                weight = [jnp.where(p > 0, 1.0, 0.0) for p in power]

                def group(g, totals):
                    totals = list(totals)
                    rows_r, rows_i = [], []
                    for s in range(8):
                        b = g * 8 + s
                        ar = ai = jnp.zeros((TILE, LANES), F32)
                        for t in range(tiles):
                            re, im = pair(k1, t, b)
                            ar = ar + re * weight[t]
                            ai = ai - im * weight[t]
                            totals[t] = totals[t] + (re * re + im * im)
                        rows_r.append(ar[:8] + ar[8:])
                        rows_i.append(ai[:8] + ai[8:])
                    store_rows(c, k, g, rows_r, rows_i)
                    return tuple(totals)

                zero = jnp.zeros((TILE, LANES), F32)
                totals = lax.fori_loop(0, blocks // 8, group, (zero,) * tiles)
                for t in range(tiles):
                    at = slice(t * TILE, (t + 1) * TILE)
                    diagonal[k1, at, :] = blocks * power[t] - totals[t]
                return carry

            lax.fori_loop(0, kc, one, 0)

        @pl.when(it > 0)
        def _():
            for copy in y_copies(c):
                copy.wait_send()
            for copy in y_copies(c, receive=True):
                copy.wait_recv()

            def one(k, carry):
                k1 = c * kc + k
                yr, yi = ([y_ref[c, k, part, t * TILE : (t + 1) * TILE, :].astype(F32)
                           for t in range(tiles)] for part in range(2))
                square = sum(a * a for a in yr + yi)
                norm[c, 0, pl.ds(k, 1), :] = jnp.sum(square, axis=0, keepdims=True)

                less = [b - a for a, b in zip(yr, yi)]
                more = [b + a for a, b in zip(yr, yi)]

                def group(g, carry):
                    rows_r, rows_i = [], []
                    for s in range(8):
                        b = g * 8 + s
                        one = two = three = None
                        for t in range(tiles):
                            re, im = pair(k1, t, b)
                            x, y, z = (re - im) * yr[t], re * less[t], im * more[t]
                            one, two, three = (x, y, z) if t == 0 else (one + x, two + y, three + z)
                        one = one[:8] + one[8:]
                        rows_r.append(one + (three[:8] + three[8:]))
                        rows_i.append(one + (two[:8] + two[8:]))
                    store_rows(c, k, g, rows_r, rows_i)
                    return carry

                lax.fori_loop(0, blocks // 8, group, 0)
                return carry

            lax.fori_loop(0, kc, one, 0)

        half_copy(c).start()
        for copy in norm_copies(c):
            copy.start()

    def add_half(it, c):
        half_copy(c).wait()
        total = local_p[c, core] + half_in[c]
        half_sum[c] = total
        half_out[c] = total.astype(BF16)
        for copy in piece_copies(c):
            copy.start()

    def add_pieces(it, c):
        for copy in piece_copies(c):
            copy.wait()
        rows = pl.ds(pl.multiple_of(z * piece_rows, piece_rows), piece_rows)
        total = half_sum[c, rows, :]
        for d in range(1, n_z):
            total = total + piece_in[c, d - 1].astype(F32)
        full_p[c, core, rows, :] = total
        for copy in gather_copies(c):
            copy.start()

    def share_half(it, c):
        for copy in gather_copies(c):
            copy.wait_send()
        for copy in gather_copies(c, receive=True):
            copy.wait_recv()
        share_copy(c).start()

    def expand(it, c):
        share_copy(c).wait_send()
        share_copy(c, receive=True).wait_recv()
        for copy in norm_copies(c):
            copy.wait()
        length = norm[c, 0]
        for d in range(1, n_chan):
            length = length + norm[c, d]
        inverse = jnp.where(it == 0, 1.0, 1.0 / jnp.sqrt(length + epsilon))
        scaled[pl.ds(3 * blocks, kc), :] = inverse

        def one(k, carry):
            k1 = c * kc + k
            inv = scaled[pl.ds(3 * blocks + k, 1), :]
            at = pl.multiple_of((k % half_k) * (2 * blocks), 2 * blocks)
            real = full_p[c, k // half_k, pl.ds(at, blocks), :] * inv
            at = pl.multiple_of(at + blocks, blocks)
            imag = full_p[c, k // half_k, pl.ds(at, blocks), :] * inv
            scaled[0:blocks, :] = real
            scaled[blocks : 2 * blocks, :] = imag - real
            scaled[2 * blocks : 3 * blocks, :] = imag + real

            def group(g, totals):
                totals = list(totals)
                for s in range(8):
                    b = g * 8 + s
                    pr, less, more = (scaled[pl.ds(i * blocks + b, 1), :] for i in range(3))
                    for t in range(tiles):
                        re, im = pair(k1, t, b)
                        totals[3 * t] = totals[3 * t] + (re + im) * pr
                        totals[3 * t + 1] = totals[3 * t + 1] + re * less
                        totals[3 * t + 2] = totals[3 * t + 2] + im * more
                return tuple(totals)

            zero = jnp.zeros((TILE, LANES), F32)
            totals = lax.fori_loop(0, blocks // 8, group, (zero,) * (3 * tiles))
            for t in range(tiles):
                at = slice(t * TILE, (t + 1) * TILE)
                usable = power_ref[k1, at, :].astype(F32) > 0
                shift = diagonal[k1, at, :] * inv
                sums = totals[3 * t] - totals[3 * t + 2], totals[3 * t] + totals[3 * t + 1]
                for part in range(2):
                    now = y_ref[c, k, part, at, :].astype(F32)
                    value = jnp.where(usable, sums[part] + shift * now, 0.0)
                    local_q[c, k, part, at, :] = value.astype(BF16)
            return carry

        lax.fori_loop(0, kc, one, 0)
        for copy in q_copies(c):
            copy.start()

    def final_copy(c, d):
        to = (me + d) % n_dev
        return remote(turned.at[c, to], out_ref.at[c, me], final_ss.at[c], final_rs.at[c],
                      section=to // n_chan, chan=to % n_chan)

    def own_copy(c):
        return pltpu.make_async_copy(turned.at[c, me], out_ref.at[c, me], own_sem.at[c])

    def final_wait(c):
        others = turned.at[c, pl.ds(0, n_dev - 1)]
        pltpu.make_async_copy(others, others, final_ss.at[c]).wait()
        others = out_ref.at[c, pl.ds(0, n_dev - 1)]
        pltpu.make_async_copy(others, others, final_rs.at[c]).wait()
        own_copy(c).wait()

    def section_sum(c, k, part):
        total = local_q[c, me_s * k_piece + k, part].astype(F32)
        for d in range(1, n_section):
            total = total + q_in[c, d - 1, k, part].astype(F32)
        return total

    def add_sections(it, c):
        for copy in q_copies(c):
            copy.wait()

        @pl.when(it < ITERS - 1)
        def _():
            for k in range(k_piece):
                for part in range(2):
                    y_ref[c, me_s * k_piece + k, part] = section_sum(c, k, part).astype(BF16)
            for copy in y_copies(c):
                copy.start()

        @pl.when(it == ITERS - 1)
        def _():
            for k in range(k_piece):
                parts = [section_sum(c, k, part) for part in range(2)]
                total = jnp.concatenate(parts, axis=0).T
                for to in range(n_dev):
                    turned[c, to, k] = total[to * share : (to + 1) * share]
            own_copy(c).start()

            @pl.loop(1, n_dev)
            def _(d):
                final_copy(c, d).start()

    barrier = pltpu.get_barrier_semaphore()

    @pl.loop(1, n_dev)
    def _(d):
        to = (me + d) % n_dev
        pl.semaphore_signal(barrier, inc=1,
                            device_id={"section": to // n_chan, "chan": to % n_chan},
                            device_id_type=pl.DeviceIdType.MESH)

    @pl.loop(0, chunks)
    def _(c):
        load(c).start()

    @pl.loop(0, chunks)
    def _(c):
        for k in range(kc):
            power = power_ref[c * kc + k].astype(F32)
            y_ref[c, k, 0] = jnp.where(power > 0, 1.0, 0.0).astype(BF16)
            y_ref[c, k, 1] = jnp.zeros((feeds, LANES), BF16)
        norm[c, 0] = jnp.zeros((kc, LANES), F32)

    pl.semaphore_wait(barrier, n_dev - 1)

    stages = [(7, add_sections), (3, add_pieces), (5, expand), (4, share_half), (1, add_half),
              (0, project)]
    span = 7
    period = max(chunks, span + 1)

    @pl.loop(0, ITERS * period + span)
    def _(slot):
        for lag, stage in stages:
            turn = slot - lag + period
            it, c = turn // period - 1, turn % period

            @pl.when((it >= 0) & (it < ITERS) & (c < chunks))
            def _():
                stage(it, c)

    @pl.loop(0, chunks)
    def _(c):
        final_wait(c)


def solve(spectra, power, n_section, n_chan):
    feeds, blocks = spectra.shape[2] * TILE, spectra.shape[3]
    kc = n_section
    chunks = OUTER // kc
    n_z = n_chan // 2
    half_rows = kc * blocks
    piece_rows = half_rows // n_z
    k_piece = kc // n_section
    n_dev = n_section * n_chan
    dma = pltpu.SemaphoreType.DMA
    per = lambda n: dma((chunks, n))
    scratch = [
        pltpu.VMEM(spectra.shape, BF16),
        pltpu.VMEM((OUTER, feeds, LANES), F32),
        pltpu.VMEM((chunks, 2, half_rows, LANES), F32),
        pltpu.VMEM((chunks, half_rows, LANES), F32),
        pltpu.VMEM((chunks, half_rows, LANES), F32),
        pltpu.VMEM((chunks, half_rows, LANES), BF16),
        pltpu.VMEM((chunks, n_z - 1, piece_rows, LANES), BF16),
        pltpu.VMEM((chunks, 2, half_rows, LANES), F32),
        pltpu.VMEM((3 * blocks + 8, LANES), F32),
        pltpu.VMEM((chunks, n_chan, kc, LANES), F32),
        pltpu.VMEM((chunks, kc, 2, feeds, LANES), BF16),
        pltpu.VMEM((chunks, n_section - 1, k_piece, 2, feeds, LANES), BF16),
        pltpu.VMEM((chunks, kc, 2, feeds, LANES), BF16),
        dma((chunks,)),
        dma((chunks,)), dma((chunks,)),
        per(n_z - 1), per(n_z - 1), per(n_z - 1), per(n_z - 1),
        dma((chunks,)), dma((chunks,)),
        per(n_chan - 1), per(n_chan - 1),
        per(n_section - 1), per(n_section - 1), per(n_section - 1), per(n_section - 1),
        pltpu.VMEM((chunks, n_dev, k_piece, LANES // n_dev, 2 * feeds), F32),
        dma((chunks,)), dma((chunks,)), dma((chunks,)),
    ]
    vmem = pl.BlockSpec(memory_space=pltpu.VMEM)
    return pl.pallas_call(
        functools.partial(solve_kernel, (n_section, n_chan, feeds, blocks, chunks, kc)),
        in_specs=[pl.BlockSpec(memory_space=pl.ANY), vmem],
        out_specs=pl.BlockSpec(memory_space=pl.ANY),
        out_shape=jax.ShapeDtypeStruct(
            (chunks, n_dev, k_piece, LANES // n_dev, 2 * feeds), F32
        ),
        scratch_shapes=scratch,
        compiler_params=pltpu.CompilerParams(
            collective_id=1, has_side_effects=True, vmem_limit_bytes=VMEM_LIMIT
        ),
    )(spectra, power)


def local(voltages, usable, auto_power):
    n_section, n_chan = lax.axis_size("section"), lax.axis_size("chan")
    power = (usable.astype(F32) * auto_power).astype(BF16)
    here = power.shape[0]
    feeds_here = power.shape[1] // n_chan
    pack = LANES // feeds_here
    power = power.reshape(pack, here // pack, n_chan, feeds_here).transpose(2, 1, 0, 3)
    power = power.reshape(n_chan, here // pack, LANES)

    spectra, power = channelize(voltages, power, n_section, n_chan)
    power = power.reshape(-1, here // pack, pack, feeds_here).transpose(0, 2, 1, 3)
    power = power.reshape(LANES, OUTER, feeds_here).transpose(1, 2, 0)
    result = solve(spectra, power, n_section, n_chan)
    chunks, k_piece = result.shape[0], result.shape[2]
    result = result.reshape(chunks, n_section, n_chan, k_piece, -1, 2, feeds_here)
    result = result.transpose(5, 4, 0, 1, 3, 2, 6).reshape(2, here, n_chan * feeds_here)
    length = jnp.sqrt(jnp.sum(result * result, axis=(0, 2)) + epsilon)
    return result / jnp.sqrt(length)[None, :, None]


def solution(mesh):
    in_specs = (
        P(None, "chan", "section"),
        P(("section", "chan"), None),
        P(("section", "chan"), None),
    )
    out_specs = P(None, ("section", "chan"), None)
    return jax.shard_map(local, mesh=mesh, in_specs=in_specs, out_specs=out_specs, check_vma=False)
```
